32 devices in a mesh: space: 8 (over z, y), slab: 4 (over x, core).
Axes of the slice: x: 2, y: 2, z: 4, core: 2. Of those that a mesh axis runs over, the one named last changes fastest.
Arguments:
- source: float32 [4, 256, 2048], P('slab', None, 'space'), may hold values from -6 to 6
- initial: float32 [64, 2048], P(None, 'space'), may hold values from -6 to 6
- inverse: float32 [256, 256], replicated, may hold values from -0.1 to 0.7, as said below
- lift: float32 [256, 384], replicated, may hold values from -0.109375 to 0.109375
- lift_time: float32 [256, 64], replicated, may hold values from -0.375 to 0.375
- links: int32 [6, 2048], P(None, 'space'), may hold values from 0 to 1791, as said below
- orient: int32 [6, 2048], P(None, 'space'), may hold values from 0 to 7
- exports: int32 [2048], P('space'), may hold values from 0 to 1535, as said below
- counts: int32 [8], P('space'), may hold values from 128 to 256, as said below
Outputs:
- state: float32 [4, 256, 2048], P('slab', None, 'space')
The draws below stay inside these ranges and needn't reach their ends.
Inputs may be any that keep to these rules, and one draw needn't show every extreme that they name: `links`: a value below 1536 is f*256 + e naming face f of a live slot e of the same partition; others are 1536 + m naming slot m of the imported neighbour traces. `exports`: each value is f*256 + e with e a live slot of that partition. `counts`: some partition holds exactly 256. `inverse`: full rank; diagonal entries between 0.5 and 0.7, off-diagonal entries of magnitude at most 0.1.
All inputs are finite; a program needn't handle non-finite values.
Results may differ from the reference program's by a relative error of at most 0.0001.
Values sent between devices are 32-bit elements; how exact they have to be, the bound alone decides.
A program may use at most 64 MiB of HBM per device.

```python
import jax
import jax.numpy as jnp
from jax import lax

ELEM_DEV = 256
ITERS = 6
PEER_CAP = 128
ELEMS = 2048
N_SPACE = 8
N_SLAB = 4


def counts_of(key):
    base = jax.random.fold_in(key, 101)
    values = jax.random.randint(base, (N_SPACE,), ELEM_DEV // 2, ELEM_DEV + 1)
    fullest = jax.random.randint(jax.random.fold_in(base, 1), (), 0, N_SPACE)
    return jnp.where(jnp.arange(N_SPACE) == fullest, ELEM_DEV, values).astype(jnp.int32)


def draw_counts(key, part):
    return counts_of(key)


def draw_links(key, part):
    live = jnp.repeat(counts_of(key), ELEM_DEV)
    keys = jax.random.split(jax.random.fold_in(key, 202), 4)
    shape = (6, ELEM_DEV * N_SPACE)
    element = jax.random.randint(keys[0], shape, 0, jnp.broadcast_to(live[None, :], shape))
    facing = jax.random.randint(keys[1], shape, 0, 6)
    remote = jax.random.randint(keys[2], shape, 0, 2 * PEER_CAP)
    crossing = jax.random.randint(keys[3], shape, 0, 4) == 0
    return jnp.where(crossing, 6 * ELEM_DEV + remote, facing * ELEM_DEV + element).astype(jnp.int32)


def draw_exports(key, part):
    live = jnp.repeat(counts_of(key), 2 * PEER_CAP)
    keys = jax.random.split(jax.random.fold_in(key, 303), 2)
    shape = (2 * PEER_CAP * N_SPACE,)
    element = jax.random.randint(keys[0], shape, 0, live)
    facing = jax.random.randint(keys[1], shape, 0, 6)
    return (facing * ELEM_DEV + element).astype(jnp.int32)


def draw_inverse(key, part):
    noise = jnp.clip(jax.random.normal(key, (256, 256), jnp.float32), -4.0, 4.0)
    return 0.6 * jnp.eye(256, dtype=jnp.float32) + 0.025 * noise


def plant(array, rng, low, largest):
    shape = array.shape
    index_at = [jax.random.randint(jax.random.fold_in(rng, axis), (), 0, shape[axis]) for axis in range(len(shape))]
    array = array.at[tuple(index_at)].set(low)
    longest = shape.index(max(shape))
    index_at[longest] = (index_at[longest] + 1) % shape[longest]
    return array.at[tuple(index_at)].set(largest)


def level_of(key, dims, shards, smallest, largest):
    factor_of, own = 1.0, jax.random.fold_in(key, 6)
    for axis_at, blocks in shards:
        steps = jnp.exp(jax.random.uniform(jax.random.fold_in(own, axis_at), (blocks,), jnp.float32, smallest / len(shards), largest / len(shards)))
        factor_of = factor_of * jnp.repeat(steps, dims[axis_at] // blocks).reshape([-1 if axis == axis_at else 1 for axis in range(len(dims))])
    return factor_of


def bell_draw(own_key, dims, width, limit, cuts=(), kind=jnp.bfloat16):
    result = width * jax.random.normal(own_key, dims, jnp.float32)
    if cuts:
        result = result * level_of(own_key, dims, cuts, -0.22, 0.18)
    return jnp.clip(result, -limit, limit).astype(kind)


def setup_inputs(seed: int = 0) -> dict:
    arg_keys = jax.random.split(jax.random.key(seed), 10)
    return {
        "source": bell_draw(arg_keys[0], (N_SLAB, 256, ELEMS), 1.0, 6.0, ((0, 4), (2, 8)), jnp.float32),
        "initial": bell_draw(arg_keys[1], (64, ELEMS), 1.0, 6.0, ((1, 8),), jnp.float32),
        "inverse": draw_inverse(jax.random.fold_in(arg_keys[9], 71), 0),
        "lift": bell_draw(arg_keys[3], (256, 384), 3072 ** -0.5, 0.109375, (), jnp.float32),
        "lift_time": bell_draw(arg_keys[4], (256, 64), 256 ** -0.5, 0.375, (), jnp.float32),
        "links": draw_links(jax.random.fold_in(arg_keys[9], 71), 0),
        "orient": plant(jax.random.randint(arg_keys[6], (6, ELEMS), 0, 8), jax.random.fold_in(arg_keys[6], 1), 0, 7).astype(jnp.int32),
        "exports": draw_exports(jax.random.fold_in(arg_keys[9], 71), 0),
        "counts": draw_counts(jax.random.fold_in(arg_keys[9], 71), 0),
    }


def face_stack(volume, axis):
    pieces = [volume[:, 0], volume[:, 3], volume[:, :, 0], volume[:, :, 3], volume[:, :, :, 0], volume[:, :, :, 3]]
    return jnp.stack(pieces, axis=axis)


def orient_traces(values, turn):
    swapped = jnp.swapaxes(values, 1, 2)
    values = jnp.where(jnp.bitwise_and(turn, 4) > 0, swapped, values)
    values = jnp.where(jnp.bitwise_and(turn, 1) > 0, jnp.flip(values, 1), values)
    values = jnp.where(jnp.bitwise_and(turn, 2) > 0, jnp.flip(values, 2), values)
    return values


def reference(source, initial, inverse, lift, lift_time, links, orient, exports, counts):
    highest = lax.Precision.HIGHEST
    parts = N_SPACE
    elems = ELEM_DEV
    peer = PEER_CAP
    live = (jnp.arange(elems, dtype=jnp.int32)[None, :] < counts[:, None]).astype(jnp.float32).reshape(1, parts * elems)
    index = links.reshape(6, parts, elems).transpose(1, 0, 2).reshape(parts, 6 * elems)
    turn = orient.reshape(6, parts, elems).transpose(1, 0, 2)
    outgo = exports.reshape(parts, 2 * peer)
    lift_three = lift.reshape(256, 64, 6)
    state = jnp.zeros((N_SLAB, 256, parts * elems), jnp.float32)
    for step in range(ITERS):
        fresh = []
        for slab in range(N_SLAB):
            volume = state[slab].reshape(4, 4, 4, 4, parts, elems)
            traces = face_stack(volume, 4).reshape(64, parts, 6 * elems)
            sent = jnp.take_along_axis(traces, outgo[None], axis=2)
            from_lower = jnp.roll(sent[:, :, peer:], 1, axis=1)
            from_upper = jnp.roll(sent[:, :, :peer], -1, axis=1)
            table = jnp.concatenate([traces, from_lower, from_upper], axis=2)
            nbr = jnp.take_along_axis(table, index[None], axis=2).reshape(4, 4, 4, parts, 6, elems)
            nbr = orient_traces(nbr, turn).reshape(64, parts, 6, elems)
            spatial = jnp.einsum('rcf,cnfe->rne', lift_three, nbr, precision=highest).reshape(256, parts * elems)
            if slab == 0:
                top = initial
            else:
                top = state[slab - 1][192:]
            rhs = source[slab] + spatial + jnp.dot(lift_time, top, precision=highest)
            fresh.append(jnp.dot(inverse, rhs, precision=highest) * live)
        state = jnp.stack(fresh)
    return state
```

```python
import functools

import jax
import jax.numpy as jnp
from jax import lax
from jax.experimental import pallas as pl
from jax.experimental.pallas import tpu as pltpu
from jax.sharding import PartitionSpec as P

ITERS = 6
LANES = 128
FACE = 64
F32, BF16 = jnp.float32, jnp.bfloat16
MESH = pl.DeviceIdType.MESH


def split(x):
    hi = x.astype(BF16)
    return hi, (x - hi.astype(F32)).astype(BF16)


def dot(a, b):
    return jnp.dot(a, b, preferred_element_type=F32)


def dot3(ah, al, b):
    bh, bl = split(b)
    return dot(ah, bh) + dot(al, bh) + dot(ah, bl)


def node_of(c):
    odd, t, b0, a0, flip = c & 1, (c >> 1) & 3, (c >> 3) & 1, (c >> 4) & 1, (c >> 5) & 1
    return t, 2 * (odd ^ flip ^ a0) + a0, 2 * (flip ^ b0) + b0


def kernel(
    n_space, n_slab,
    source_hbm, initial_hbm, inverse_hbm, lift_hbm, lift_time_hbm, links_hbm, orient_hbm, exports_hbm, counts_hbm, out,
    source, initial, inverse, lift, lift_time, links, orient, exports, counts, load_sem,
    weight, bias, rhs, traces, local, send, top_send, recv, top_recv, send_sem, recv_sem,
):
    size, elems = source.shape[1:]
    faces = links.shape[0]
    wide = faces * FACE
    peer = exports.shape[1]
    tiles, peer_tiles = elems // LANES, peer // LANES
    rows = wide + FACE

    space, slab = lax.axis_index("space"), lax.axis_index("slab")
    upper, lower = lax.rem(space + 1, n_space), lax.rem(space + n_space - 1, n_space)
    odd = lax.rem(space, 2)
    has_prev, has_next = slab > 0, slab < n_slab - 1

    barrier = pltpu.get_barrier_semaphore()
    before, after = lax.rem(slab + n_slab - 1, n_slab), lax.rem(slab + 1, n_slab)
    peers = ((lower, slab), (upper, slab), (space, before), (space, after))
    for device in peers:
        pl.semaphore_signal(barrier, inc=1, device_id=device, device_id_type=MESH)

    pairs = (
        (inverse_hbm, inverse), (source_hbm, source), (lift_time_hbm, lift_time), (initial_hbm, initial),
        (counts_hbm, counts), (exports_hbm, exports), (links_hbm, links), (lift_hbm, lift), (orient_hbm, orient),
    )
    loads = [pltpu.make_async_copy(src, dst, load_sem.at[k]) for k, (src, dst) in enumerate(pairs)]
    for load in loads:
        load.start()

    row = lax.broadcasted_iota(jnp.int32, (rows, size), 0)
    face = row >> 6
    t, a, b = node_of(row & 63)
    at = jnp.where(face < 2, 4 * a + b, jnp.where(face < 4, 16 * a + b, 16 * a + 4 * b))
    step_up = jnp.where(face < 2, 48, jnp.where(face < 4, 12, 3))
    at = jnp.where(face < 6, 64 * t + at + (face & 1) * step_up, size - FACE + row - wide)
    pick = (at == lax.broadcasted_iota(jnp.int32, (rows, size), 1)).astype(BF16)
    for load in loads[:5]:
        load.wait()
    live = (lax.broadcasted_iota(jnp.int32, (1, elems), 1) < counts[0]).astype(F32)
    inv_hi, inv_lo = split(inverse[...])
    inv_hi = jnp.concatenate([dot(pick, inv_hi).astype(BF16), inv_hi], axis=0)
    inv_lo = jnp.concatenate([dot(pick, inv_lo).astype(BF16), inv_lo], axis=0)
    first_top = jnp.where(slab == 0, initial[...], 0.0)
    lt_hi, lt_lo = split(lift_time[...].T)
    bias[...] = dot3(inv_hi, inv_lo, source[0] + dot3(lt_hi, lt_lo, first_top))
    traces[...] = bias[:rows] * live

    pl.semaphore_wait(barrier, len(peers))

    def copies(n):
        def copy(src, dst, k, device):
            return pltpu.make_async_remote_copy(
                src_ref=src, dst_ref=dst, send_sem=send_sem.at[n, k], recv_sem=recv_sem.at[n, k],
                device_id=device, device_id_type=MESH,
            )
        far = copy(send.at[n, odd], recv.at[n, 1 - odd], 0, (jnp.where(odd == 1, upper, lower), slab))
        near = copy(send.at[n, 1 - odd], recv.at[n, odd], 1, (jnp.where(odd == 1, lower, upper), slab))
        late = copy(top_send.at[n], top_recv.at[n], 2, (space, after))
        return far, near, late

    def gather(blocks, column, first, acc):
        lane = jnp.broadcast_to(column & (LANES - 1), acc.shape)
        tile = jnp.broadcast_to(column >> 7, acc.shape)
        for k, block in enumerate(blocks):
            got = jnp.take_along_axis(block, lane, axis=1, mode="promise_in_bounds")
            acc = jnp.where(tile == first + k, got, acc)
        return acc

    def own_blocks():
        return [
            traces[f * FACE:(f + 1) * FACE, h * LANES:(h + 1) * LANES] for f in range(faces) for h in range(tiles)
        ]

    def turned(x, code):
        groups = [x[8 * q:8 * q + 8] for q in range(8)]
        code = jnp.broadcast_to(code, groups[0].shape)
        odd = (lax.broadcasted_iota(jnp.int32, code.shape, 0) & 1) > 0
        swap, back_a, back_b = (code & 4) > 0, (code & 1) > 0, (code & 2) > 0
        swap_odd, swap_even = swap & odd, swap & ~odd
        mid = []
        for q in range(8):
            flip, a0, b0 = q >> 2, (q >> 1) & 1, q & 1
            even_at, odd_at = flip * 4 + b0 * 2 + a0, (1 - flip) * 4 + b0 * 2 + a0
            mid.append(jnp.where(swap_odd, groups[odd_at], jnp.where(swap_even, groups[even_at], groups[q])))
        mid = [jnp.where(back_a, mid[q ^ 2], mid[q]) for q in range(8)]
        return jnp.concatenate([jnp.where(back_b, mid[q ^ 1], mid[q]) for q in range(8)], axis=0)

    def send_out(n):
        zero = jnp.zeros((FACE, LANES), F32)
        blocks = own_blocks()
        far, near, late = copies(n)
        for half, copy in ((odd, far), (1 - odd, near)):
            for h in range(peer_tiles):
                cols = slice(h * LANES, (h + 1) * LANES)
                send[n, half, :, cols] = gather(blocks, exports[pl.ds(half, 1), cols], 0, zero)
            copy.start()
        top_send[n] = traces[wide:]
        pl.when(has_next)(late.start)

    def gather_own():
        zero = jnp.zeros((FACE, LANES), F32)
        blocks = own_blocks()
        for f in range(faces):
            for h in range(tiles):
                cols = slice(h * LANES, (h + 1) * LANES)
                local[f * FACE:(f + 1) * FACE, cols] = gather(blocks, links[f:f + 1, cols], 0, zero)

    def take_in(n):
        far, near, late = copies(n)

        def blocks(side):
            return [recv[n, side, :, h * LANES:(h + 1) * LANES] for h in range(peer_tiles)]

        near.wait_recv()
        for f in range(faces):
            for h in range(tiles):
                at, cols = slice(f * FACE, (f + 1) * FACE), slice(h * LANES, (h + 1) * LANES)
                first = faces * tiles + (1 - odd) * peer_tiles
                local[at, cols] = gather(blocks(1 - odd), links[f:f + 1, cols], first, local[at, cols])
        far.wait_recv()
        for f in range(faces):
            for h in range(tiles):
                at, cols = slice(f * FACE, (f + 1) * FACE), slice(h * LANES, (h + 1) * LANES)
                first = faces * tiles + odd * peer_tiles
                x = gather(blocks(odd), links[f:f + 1, cols], first, local[at, cols])
                hi, lo = split(turned(x, orient[f:f + 1, cols]))
                rhs[at, cols] = hi
                rhs[wide + f * FACE:wide + (f + 1) * FACE, cols] = hi
                rhs[2 * wide + f * FACE:2 * wide + (f + 1) * FACE, cols] = lo

        @pl.when(has_prev)
        def _():
            late.wait_recv()
            hi, lo = split(top_recv[n])
            for k, piece in enumerate((hi, hi, lo, lo)):
                rhs[3 * wide + k * FACE:3 * wide + (k + 1) * FACE, :] = piece

    def sent(n):
        far, near, late = copies(n)
        far.wait_send()
        near.wait_send()
        pl.when(has_next)(late.wait_send)

    loads[5].wait()
    send_out(0)
    for load in loads[6:]:
        load.wait()
    gather_own()

    place = lax.broadcasted_iota(jnp.int32, (wide, wide), 1)
    t, a, b = node_of(place & 63)
    at = (16 * t + 4 * a + b) * faces + (place >> 6)
    order = (at == lax.broadcasted_iota(jnp.int32, (wide, wide), 0)).astype(BF16)
    lift_hi, lift_lo = split(lift[...])
    lift_hi, lift_lo = dot(lift_hi, order).astype(BF16), dot(lift_lo, order).astype(BF16)
    part = dot(inv_hi, lift_hi) + dot(inv_lo, lift_hi) + dot(inv_hi, lift_lo)
    hi, lo = split(part)
    weight[:, :wide] = hi
    weight[:, wide:2 * wide] = lo
    weight[:, 2 * wide:3 * wide] = hi
    part = dot(inv_hi, lt_hi) + dot(inv_lo, lt_hi) + dot(inv_hi, lt_lo)
    hi, lo = split(part)
    both = jnp.concatenate([hi, lo], axis=1)
    weight[:, 3 * wide:3 * wide + 2 * FACE] = both
    weight[:, 3 * wide + 2 * FACE:] = both
    rhs[3 * wide:] = jnp.zeros((4 * FACE, elems), BF16)

    def step(n, carry):
        @pl.when(n > 0)
        def _():
            send_out(n)
            gather_own()

        take_in(n)
        sent(n)
        traces[...] = (dot(weight[:rows], rhs[...]) + bias[:rows]) * live
        return carry

    lax.fori_loop(0, ITERS - 2, step, 0)
    send_out(ITERS - 2)
    gather_own()
    take_in(ITERS - 2)
    out[0] = (dot(weight[rows:], rhs[...]) + bias[rows:]) * live
    sent(ITERS - 2)


def body(n_space, n_slab, source, initial, inverse, lift, lift_time, links, orient, exports, counts):
    size, elems = source.shape[1:]
    wide = links.shape[0] * FACE
    rows, depth = wide + FACE, 3 * wide + 4 * FACE
    peer = exports.shape[0] // 2
    hops = ITERS - 1
    operands = (source, initial, inverse, lift, lift_time.T, links, orient, exports.reshape(2, peer), counts)
    return pl.pallas_call(
        functools.partial(kernel, n_space, n_slab),
        out_shape=pltpu.VMEM(source.shape, F32),
        in_specs=[pl.BlockSpec(memory_space=pltpu.HBM)] * 9,
        out_specs=pl.BlockSpec(memory_space=pltpu.VMEM),
        scratch_shapes=[
            *(pltpu.VMEM(x.shape, x.dtype) for x in operands[:8]),
            pltpu.SMEM(counts.shape, counts.dtype),
            pltpu.SemaphoreType.DMA((9,)),
            pltpu.VMEM((rows + size, depth), BF16),
            pltpu.VMEM((rows + size, elems), F32),
            pltpu.VMEM((depth, elems), BF16),
            pltpu.VMEM((rows, elems), F32),
            pltpu.VMEM((wide, elems), F32),
            pltpu.VMEM((hops, 2, FACE, peer), F32),
            pltpu.VMEM((hops, FACE, elems), F32),
            pltpu.VMEM((hops, 2, FACE, peer), F32),
            pltpu.VMEM((hops, FACE, elems), F32),
            pltpu.SemaphoreType.DMA((hops, 3)),
            pltpu.SemaphoreType.DMA((hops, 3)),
        ],
        compiler_params=pltpu.CompilerParams(collective_id=0, has_side_effects=True, vmem_limit_bytes=60000 * 1024),
    )(*operands)


def solution(mesh):
    return jax.shard_map(
        functools.partial(body, mesh.shape["space"], mesh.shape["slab"]),
        mesh=mesh,
        in_specs=(
            P("slab", None, "space"),
            P(None, "space"),
            P(),
            P(),
            P(),
            P(None, "space"),
            P(None, "space"),
            P("space"),
            P("space"),
        ),
        out_specs=P("slab", None, "space"),
        check_vma=False,
    )
```

```python
import functools

import jax
import jax.numpy as jnp
from jax import lax
from jax.experimental import pallas as pl
from jax.experimental.pallas import tpu as pltpu
from jax.sharding import PartitionSpec as P

ITERS = 6
LANES = 128
FACE = 64
F32, BF16 = jnp.float32, jnp.bfloat16
MESH = pl.DeviceIdType.MESH


def split(x):
    hi = x.astype(BF16)
    return hi, (x - hi.astype(F32)).astype(BF16)


def dot(a, b):
    return jnp.dot(a, b, preferred_element_type=F32)


def dot3(ah, al, b):
    bh, bl = split(b)
    return dot(ah, bh) + dot(al, bh) + dot(ah, bl)


def fold(c):
    return (c >> 1) ^ (c & 1)


def node_of(c):
    odd, t, b0, a0, flip = c & 1, (c >> 1) & 3, (c >> 3) & 1, (c >> 4) & 1, (c >> 5) & 1
    return t, 2 * (odd ^ flip ^ a0) + a0, 2 * (flip ^ b0) + b0


def point_of(group, odd):
    k, j, i0 = group & 3, (group >> 2) & 3, group >> 4
    return 16 * (2 * (odd ^ fold(j) ^ fold(k) ^ i0) + i0) + 4 * j + k


def kernel(
    n_space, n_slab,
    source_hbm, initial_hbm, inverse_hbm, lift_hbm, lift_time_hbm, links_hbm, orient_hbm, exports_hbm, counts_hbm, out,
    source, initial, inverse, lift, lift_time, links, orient, exports, counts, load_sem,
    weight_hi, weight_lo, bias, rhs_hi, rhs_lo, state, local, send, top_send, recv, top_recv, send_sem, recv_sem,
):
    size, elems = source.shape[1:]
    faces = links.shape[0]
    wide = faces * FACE
    peer = exports.shape[1]
    tiles, peer_tiles = elems // LANES, peer // LANES
    hops = ITERS - 1

    space, slab = lax.axis_index("space"), lax.axis_index("slab")
    upper, lower = lax.rem(space + 1, n_space), lax.rem(space + n_space - 1, n_space)
    odd = lax.rem(space, 2)
    has_prev, has_next = slab > 0, slab < n_slab - 1

    barrier = pltpu.get_barrier_semaphore()
    before, after = lax.rem(slab + n_slab - 1, n_slab), lax.rem(slab + 1, n_slab)
    peers = ((lower, slab), (upper, slab), (space, before), (space, after))
    for device in peers:
        pl.semaphore_signal(barrier, inc=1, device_id=device, device_id_type=MESH)

    pairs = (
        (inverse_hbm, inverse), (source_hbm, source), (lift_time_hbm, lift_time), (initial_hbm, initial),
        (counts_hbm, counts), (exports_hbm, exports), (links_hbm, links), (lift_hbm, lift), (orient_hbm, orient),
    )
    loads = [pltpu.make_async_copy(src, dst, load_sem.at[k]) for k, (src, dst) in enumerate(pairs)]
    for load in loads:
        load.start()

    row = lax.broadcasted_iota(jnp.int32, (size, size), 0)
    at = 64 * ((row >> 1) & 3) + point_of(row >> 3, row & 1)
    pick = (at == lax.broadcasted_iota(jnp.int32, (size, size), 1)).astype(BF16)
    for load in loads[:5]:
        load.wait()
    live = (lax.broadcasted_iota(jnp.int32, (1, elems), 1) < counts[0]).astype(F32)
    inv_hi, inv_lo = split(inverse[...])
    own_hi, own_lo = dot(pick, inv_hi).astype(BF16), dot(pick, inv_lo).astype(BF16)
    first_top = jnp.where(slab == 0, initial[...], 0.0)
    lt_hi, lt_lo = split(lift_time[...].T)
    total = source[0] + dot3(lt_hi, lt_lo, first_top)
    first = dot3(own_hi, own_lo, total)
    bias[:size] = first
    state[...] = first * live

    def copies(n):
        def copy(src, dst, k, device):
            return pltpu.make_async_remote_copy(
                src_ref=src, dst_ref=dst, send_sem=send_sem.at[n, k], recv_sem=recv_sem.at[n, k],
                device_id=device, device_id_type=MESH,
            )
        far = copy(send.at[n, odd], recv.at[n, 1 - odd], 0, (jnp.where(odd == 1, upper, lower), slab))
        near = copy(send.at[n, 1 - odd], recv.at[n, odd], 1, (jnp.where(odd == 1, lower, upper), slab))
        late = copy(top_send.at[n], top_recv.at[n], 2, (space, after))
        return far, near, late

    def spread(column):
        column = jnp.broadcast_to(column, (8, LANES))
        return column & (LANES - 1), column >> 7

    def taken(x, lane):
        return jnp.take_along_axis(x, lane, axis=1, mode="promise_in_bounds")

    def from_state(column):
        lane, tile = spread(column)
        face, part = lax.div(tile, tiles), lax.rem(tile, tiles)
        parts = [part == h for h in range(1, tiles)]
        at_face = [face == f for f in range(1, faces)]
        groups = []
        for v in range(size // 8):
            got = taken(state[8 * v:8 * v + 8, :LANES], lane)
            for h in range(1, tiles):
                got = jnp.where(parts[h - 1], taken(state[8 * v:8 * v + 8, h * LANES:(h + 1) * LANES], lane), got)
            groups.append(got)
        row_odd = (lax.broadcasted_iota(jnp.int32, (8, LANES), 0) & 1) > 0

        def group(i0, j, k):
            return groups[16 * i0 + 4 * j + k]

        result = []
        for q in range(8):
            flip, a0, b0 = q >> 2, (q >> 1) & 1, q & 1
            b = 2 * (flip ^ b0) + b0
            low, high = 2 * (flip ^ a0) + a0, 2 * (1 ^ flip ^ a0) + a0
            sides = [jnp.where(row_odd, group(i0, high, b), group(i0, low, b)) for i0 in range(2)]
            sides += [group(a0, 0, b), group(a0, 3, b), group(a0, b, 0), group(a0, b, 3)]
            x = sides[0]
            for f in range(1, faces):
                x = jnp.where(at_face[f - 1], sides[f], x)
            result.append(x)
        return result

    def from_peer(n, side, first, column, held):
        lane, tile = spread(column)
        result = held
        for h in range(peer_tiles):
            here = tile == first + h
            result = [
                jnp.where(here, taken(recv[n, side, 8 * q:8 * q + 8, h * LANES:(h + 1) * LANES], lane), result[q])
                for q in range(8)
            ]
        return result

    def turned(groups, code):
        code = jnp.broadcast_to(code, groups[0].shape)
        odd = (lax.broadcasted_iota(jnp.int32, code.shape, 0) & 1) > 0
        swap, back_a, back_b = (code & 4) > 0, (code & 1) > 0, (code & 2) > 0
        swap_odd, swap_even = swap & odd, swap & ~odd
        mid = []
        for q in range(8):
            flip, a0, b0 = q >> 2, (q >> 1) & 1, q & 1
            even_at, odd_at = flip * 4 + b0 * 2 + a0, (1 - flip) * 4 + b0 * 2 + a0
            mid.append(jnp.where(swap_odd, groups[odd_at], jnp.where(swap_even, groups[even_at], groups[q])))
        mid = [jnp.where(back_a, mid[q ^ 2], mid[q]) for q in range(8)]
        return [jnp.where(back_b, mid[q ^ 1], mid[q]) for q in range(8)]

    def send_out(n):
        far, near, late = copies(n)
        for half, copy in ((odd, far), (1 - odd, near)):
            for h in range(peer_tiles):
                cols = slice(h * LANES, (h + 1) * LANES)
                got = from_state(exports[pl.ds(half, 1), cols])
                for q in range(8):
                    send[n, half, 8 * q:8 * q + 8, cols] = got[q]
            copy.start()
        sub = lax.broadcasted_iota(jnp.int32, (8, elems), 0) >> 1
        for w in range(8):
            pack = state[32 * w + 24:32 * w + 32]
            for m in range(3):
                pack = jnp.where(sub == m, pltpu.roll(state[32 * w + 8 * m:32 * w + 8 * m + 8], 2 * m + 2, 0), pack)
            top_send[n, 8 * w:8 * w + 8] = pack
        pl.when(has_next)(late.start)

    spots = [(f, h) for f in range(faces) for h in range(tiles)]

    def gather_own():
        for f, h in spots:
            cols = slice(h * LANES, (h + 1) * LANES)
            got = from_state(links[f:f + 1, cols])
            for q in range(8):
                local[f * FACE + 8 * q:f * FACE + 8 * q + 8, cols] = got[q]

    def held(f, cols):
        return [local[f * FACE + 8 * q:f * FACE + 8 * q + 8, cols] for q in range(8)]

    def take_in(n):
        far, near, late = copies(n)
        near.wait_recv()
        for f, h in spots:
            cols = slice(h * LANES, (h + 1) * LANES)
            first = faces * tiles + (1 - odd) * peer_tiles
            got = from_peer(n, 1 - odd, first, links[f:f + 1, cols], held(f, cols))
            for q in range(8):
                local[f * FACE + 8 * q:f * FACE + 8 * q + 8, cols] = got[q]

        @pl.when(has_prev)
        def _():
            late.wait_recv()
            rhs_hi[wide:], rhs_lo[wide:] = split(top_recv[n])

        far.wait_recv()
        for f, h in spots:
            at, cols = slice(f * FACE, (f + 1) * FACE), slice(h * LANES, (h + 1) * LANES)
            first = faces * tiles + odd * peer_tiles
            got = from_peer(n, odd, first, links[f:f + 1, cols], held(f, cols))
            hi, lo = split(jnp.concatenate(turned(got, orient[f:f + 1, cols]), axis=0))
            rhs_hi[at, cols] = hi
            rhs_lo[at, cols] = lo

    def solved(at):
        x_hi, x_lo = rhs_hi[...], rhs_lo[...]
        return (dot(jnp.concatenate([weight_hi[at], weight_lo[at], weight_hi[at]], axis=1), jnp.concatenate([x_hi, x_hi, x_lo], axis=0)) + bias[at]) * live

    for load in loads[5:6]:
        load.wait()
    pl.semaphore_wait(barrier, len(peers))
    send_out(0)
    for load in loads[6:]:
        load.wait()

    place = lax.broadcasted_iota(jnp.int32, (wide, wide), 1)
    t, a, b = node_of(place & 63)
    at = (16 * t + 4 * a + b) * faces + (place >> 6)
    order = (at == lax.broadcasted_iota(jnp.int32, (wide, wide), 0)).astype(BF16)
    place = lax.broadcasted_iota(jnp.int32, (FACE, FACE), 1)
    top_order = (point_of(place >> 1, place & 1) == lax.broadcasted_iota(jnp.int32, (FACE, FACE), 0)).astype(BF16)
    lift_hi, lift_lo = split(lift[...])
    lift_hi = jnp.concatenate([dot(lift_hi, order).astype(BF16), dot(lt_hi, top_order).astype(BF16)], axis=1)
    lift_lo = jnp.concatenate([dot(lift_lo, order).astype(BF16), dot(lt_lo, top_order).astype(BF16)], axis=1)
    inv_hi, inv_lo = jnp.concatenate([own_hi, inv_hi], axis=0), jnp.concatenate([own_lo, inv_lo], axis=0)
    part = dot(inv_hi, lift_hi) + dot(inv_lo, lift_hi) + dot(inv_hi, lift_lo)
    weight_hi[...], weight_lo[...] = split(part)
    bias[size:] = dot3(inv_hi[size:], inv_lo[size:], source[0] + dot3(lt_hi, lt_lo, first_top))
    rhs_hi[wide:] = jnp.zeros((FACE, elems), BF16)
    rhs_lo[wide:] = jnp.zeros((FACE, elems), BF16)

    def step(n, carry):
        gather_own()
        take_in(n)
        state[...] = solved(slice(0, size))
        send_out(n + 1)
        return carry

    lax.fori_loop(0, hops - 1, step, 0)
    gather_own()
    take_in(hops - 1)
    out[0] = solved(slice(size, 2 * size))

    def sent(n, carry):
        far, near, late = copies(n)
        far.wait_send()
        near.wait_send()
        pl.when(has_next)(late.wait_send)
        return carry

    lax.fori_loop(0, hops, sent, 0)


def body(n_space, n_slab, source, initial, inverse, lift, lift_time, links, orient, exports, counts):
    size, elems = source.shape[1:]
    wide = links.shape[0] * FACE
    depth = wide + FACE
    peer = exports.shape[0] // 2
    hops = ITERS - 1
    operands = (source, initial, inverse, lift, lift_time.T, links, orient, exports.reshape(2, peer), counts)
    return pl.pallas_call(
        functools.partial(kernel, n_space, n_slab),
        out_shape=pltpu.VMEM(source.shape, F32),
        in_specs=[pl.BlockSpec(memory_space=pltpu.HBM)] * 9,
        out_specs=pl.BlockSpec(memory_space=pltpu.VMEM),
        scratch_shapes=[
            *(pltpu.VMEM(x.shape, x.dtype) for x in operands[:8]),
            pltpu.SMEM(counts.shape, counts.dtype),
            pltpu.SemaphoreType.DMA((9,)),
            pltpu.VMEM((2 * size, depth), BF16),
            pltpu.VMEM((2 * size, depth), BF16),
            pltpu.VMEM((2 * size, elems), F32),
            pltpu.VMEM((depth, elems), BF16),
            pltpu.VMEM((depth, elems), BF16),
            pltpu.VMEM((size, elems), F32),
            pltpu.VMEM((wide, elems), F32),
            pltpu.VMEM((hops, 2, FACE, peer), F32),
            pltpu.VMEM((hops, FACE, elems), F32),
            pltpu.VMEM((hops, 2, FACE, peer), F32),
            pltpu.VMEM((hops, FACE, elems), F32),
            pltpu.SemaphoreType.DMA((hops, 3)),
            pltpu.SemaphoreType.DMA((hops, 3)),
        ],
        compiler_params=pltpu.CompilerParams(collective_id=0, has_side_effects=True, vmem_limit_bytes=60000 * 1024),
    )(*operands)


def solution(mesh):
    return jax.shard_map(
        functools.partial(body, mesh.shape["space"], mesh.shape["slab"]),
        mesh=mesh,
        in_specs=(
            P("slab", None, "space"),
            P(None, "space"),
            P(),
            P(),
            P(),
            P(None, "space"),
            P(None, "space"),
            P("space"),
            P("space"),
        ),
        out_specs=P("slab", None, "space"),
        check_vma=False,
    )
```

```python
import functools

import jax
import jax.numpy as jnp
from jax import lax
from jax.experimental import pallas as pl
from jax.experimental.pallas import tpu as pltpu
from jax.sharding import PartitionSpec as P

ITERS = 6
LANES = 128
FACE = 64
LAG = 2
F32, BF16 = jnp.float32, jnp.bfloat16
MESH = pl.DeviceIdType.MESH


def split(x):
    hi = x.astype(BF16)
    return hi, (x - hi.astype(F32)).astype(BF16)


def dot(a, b):
    return jnp.dot(a, b, preferred_element_type=F32)


def dot3(ah, al, b):
    bh, bl = split(b)
    return dot(ah, bh) + dot(al, bh) + dot(ah, bl)


def fold(c):
    return (c >> 1) ^ (c & 1)


def node_of(c):
    odd, t, b0, a0, flip = c & 1, (c >> 1) & 3, (c >> 3) & 1, (c >> 4) & 1, (c >> 5) & 1
    return t, 2 * (odd ^ flip ^ a0) + a0, 2 * (flip ^ b0) + b0


def point_of(group, odd):
    k, j, i0 = group & 3, (group >> 2) & 3, group >> 4
    return 16 * (2 * (odd ^ fold(j) ^ fold(k) ^ i0) + i0) + 4 * j + k


def kernel(
    n_space, n_slab,
    source_hbm, initial_hbm, inverse_hbm, lift_hbm, lift_time_hbm, links_hbm, orient_hbm, exports_hbm, counts_hbm, out,
    source, initial, inverse, lift, lift_time, links, orient, exports, counts, load_sem,
    weight_hi, weight_lo, bias, rhs_hi, rhs_lo, state, local, send, top_send, recv, top_recv, send_sem, recv_sem,
    notes, twin_notes, twin_bias, twin_state, twin_local, feed, twin_top, bulk_send, bulk_recv,
):
    size, elems = source.shape[1:]
    faces = links.shape[0]
    wide = faces * FACE
    peer = exports.shape[1]
    tiles, peer_tiles = elems // LANES, peer // LANES
    hops = ITERS - 1

    space, slab = lax.axis_index("space"), lax.axis_index("slab")
    upper, lower = lax.rem(space + 1, n_space), lax.rem(space + n_space - 1, n_space)
    odd = lax.rem(space, 2)
    has_prev, has_next = slab > 0, slab < n_slab - 1
    even, edge = lax.rem(slab, 2) == 0, space == n_space - 1
    host, home = even & (space == 0), even & edge
    feeder, teller = even & (space == n_space - 2), ~even & edge & has_next

    barrier = pltpu.get_barrier_semaphore()
    before, after = lax.rem(slab + n_slab - 1, n_slab), lax.rem(slab + 1, n_slab)
    peers = ((lower, slab), (upper, slab), (space, before), (space, after))
    for device in peers:
        pl.semaphore_signal(barrier, inc=1, device_id=device, device_id_type=MESH)

    @pl.when(host)
    def _():
        pl.semaphore_signal(barrier, inc=1, device_id=(n_space - 2, slab), device_id_type=MESH)

    @pl.when(host & has_prev)
    def _():
        pl.semaphore_signal(barrier, inc=1, device_id=(n_space - 1, before), device_id_type=MESH)

    pairs = (
        (inverse_hbm, inverse), (source_hbm, source), (lift_time_hbm, lift_time), (initial_hbm, initial),
        (counts_hbm, counts), (exports_hbm, exports), (links_hbm, links), (lift_hbm, lift), (orient_hbm, orient),
    )
    loads = [pltpu.make_async_copy(src, dst, load_sem.at[k]) for k, (src, dst) in enumerate(pairs)]
    for load in loads:
        load.start()

    row = lax.broadcasted_iota(jnp.int32, (size, size), 0)
    at = 64 * ((row >> 1) & 3) + point_of(row >> 3, row & 1)
    pick = (at == lax.broadcasted_iota(jnp.int32, (size, size), 1)).astype(BF16)
    for load in loads[:5]:
        load.wait()
    live = (lax.broadcasted_iota(jnp.int32, (1, elems), 1) < counts[0]).astype(F32)
    inv_hi, inv_lo = split(inverse[...])
    own_hi, own_lo = dot(pick, inv_hi).astype(BF16), dot(pick, inv_lo).astype(BF16)
    first_top = jnp.where(slab == 0, initial[...], 0.0)
    lt_hi, lt_lo = split(lift_time[...].T)
    total = source[0] + dot3(lt_hi, lt_lo, first_top)
    first = dot3(own_hi, own_lo, total)
    bias[:size] = first
    state[...] = first * live

    def copy(src, dst, sems, at, device):
        return pltpu.make_async_remote_copy(
            src_ref=src, dst_ref=dst, send_sem=sems[0].at[at], recv_sem=sems[1].at[at],
            device_id=device, device_id_type=MESH,
        )

    sems, bulk_sems = (send_sem, recv_sem), (bulk_send, bulk_recv)

    def far(n):
        return copy(send.at[n, odd], recv.at[n, 1 - odd], sems, (n, 0), (jnp.where(odd == 1, upper, lower), slab))

    def near(n):
        return copy(send.at[n, 1 - odd], recv.at[n, odd], sems, (n, 1), (jnp.where(odd == 1, lower, upper), slab))

    def late(n):
        return copy(top_send.at[n], top_recv.at[n], sems, (n, 2), (space, after))

    def feed_twin(n):
        return copy(send.at[n, 1 - odd], feed.at[n], sems, (n, 3), (0, slab))

    def tell_twin(n):
        return copy(top_send.at[n], twin_top.at[n], sems, (n, 4), (0, after))

    def bulk():
        return [copy(x, y, bulk_sems, k, (0, slab)) for k, (x, y) in enumerate(((notes, twin_notes), (bias.at[:size], twin_bias)))]

    def spread(column):
        column = jnp.broadcast_to(column, (8, LANES))
        return column & (LANES - 1), column >> 7

    def taken(x, lane):
        return jnp.take_along_axis(x, lane, axis=1, mode="promise_in_bounds")

    def from_state(state, column):
        lane, tile = spread(column)
        face, part = lax.div(tile, tiles), lax.rem(tile, tiles)
        parts = [part == h for h in range(1, tiles)]
        at_face = [face == f for f in range(1, faces)]
        groups = []
        for v in range(size // 8):
            got = taken(state[8 * v:8 * v + 8, :LANES], lane)
            for h in range(1, tiles):
                got = jnp.where(parts[h - 1], taken(state[8 * v:8 * v + 8, h * LANES:(h + 1) * LANES], lane), got)
            groups.append(got)
        row_odd = (lax.broadcasted_iota(jnp.int32, (8, LANES), 0) & 1) > 0

        def group(i0, j, k):
            return groups[16 * i0 + 4 * j + k]

        result = []
        for q in range(8):
            flip, a0, b0 = q >> 2, (q >> 1) & 1, q & 1
            b = 2 * (flip ^ b0) + b0
            low, high = 2 * (flip ^ a0) + a0, 2 * (1 ^ flip ^ a0) + a0
            sides = [jnp.where(row_odd, group(i0, high, b), group(i0, low, b)) for i0 in range(2)]
            sides += [group(a0, 0, b), group(a0, 3, b), group(a0, b, 0), group(a0, b, 3)]
            x = sides[0]
            for f in range(1, faces):
                x = jnp.where(at_face[f - 1], sides[f], x)
            result.append(x)
        return result

    def from_peer(block, first, column, held):
        lane, tile = spread(column)
        result = held
        for h in range(peer_tiles):
            here = tile == first + h
            result = [
                jnp.where(here, taken(block[8 * q:8 * q + 8, h * LANES:(h + 1) * LANES], lane), result[q])
                for q in range(8)
            ]
        return result

    def turned(groups, code):
        code = jnp.broadcast_to(code, groups[0].shape)
        odd = (lax.broadcasted_iota(jnp.int32, code.shape, 0) & 1) > 0
        swap, back_a, back_b = (code & 4) > 0, (code & 1) > 0, (code & 2) > 0
        swap_odd, swap_even = swap & odd, swap & ~odd
        mid = []
        for q in range(8):
            flip, a0, b0 = q >> 2, (q >> 1) & 1, q & 1
            even_at, odd_at = flip * 4 + b0 * 2 + a0, (1 - flip) * 4 + b0 * 2 + a0
            mid.append(jnp.where(swap_odd, groups[odd_at], jnp.where(swap_even, groups[even_at], groups[q])))
        mid = [jnp.where(back_a, mid[q ^ 2], mid[q]) for q in range(8)]
        return [jnp.where(back_b, mid[q ^ 1], mid[q]) for q in range(8)]

    def put(ref, spot, groups):
        f, h = spot
        for q in range(8):
            ref[f * FACE + 8 * q:f * FACE + 8 * q + 8, h * LANES:(h + 1) * LANES] = groups[q]

    def held(ref, spot):
        f, h = spot
        return [ref[f * FACE + 8 * q:f * FACE + 8 * q + 8, h * LANES:(h + 1) * LANES] for q in range(8)]

    def at_spot(ref, spot, base=0):
        f, h = spot
        return ref[base + f:base + f + 1, h * LANES:(h + 1) * LANES]

    spots = [(f, h) for f in range(faces) for h in range(tiles)]
    outer = faces * tiles

    def pack_top(state, dst):
        sub = lax.broadcasted_iota(jnp.int32, (8, elems), 0) >> 1
        for w in range(8):
            pack = state[32 * w + 24:32 * w + 32]
            for m in range(3):
                pack = jnp.where(sub == m, pltpu.roll(state[32 * w + 8 * m:32 * w + 8 * m + 8], 2 * m + 2, 0), pack)
            dst[8 * w:8 * w + 8] = pack

    def by_wire(edge_kind, n):
        return jnp.logical_or(jnp.logical_not(edge_kind), n < LAG)

    def send_out(n):
        for half in (odd, 1 - odd):
            for h in range(peer_tiles):
                cols = slice(h * LANES, (h + 1) * LANES)
                put(send.at[n, half], (0, h), from_state(state, exports[pl.ds(half, 1), cols]))
            if half is odd:
                pl.when(by_wire(home, n))(lambda: far(n).start())
        near(n).start()
        pl.when(feeder & (n < hops - 1))(lambda: feed_twin(n).start())
        pack_top(state, top_send.at[n])
        pl.when(has_next)(lambda: late(n).start())
        pl.when(teller & (n < hops - 1))(lambda: tell_twin(n).start())

    def gather_own(state, local, links):
        for spot in spots:
            put(local, spot, from_state(state, at_spot(links, spot)))

    def add_near(local, links, block, first):
        for spot in spots:
            put(local, spot, from_peer(block, first, at_spot(links, spot), held(local, spot)))

    def add_far(local, links, orient, base, block, first):
        for spot in spots:
            f, h = spot
            at, cols = slice(f * FACE, (f + 1) * FACE), slice(h * LANES, (h + 1) * LANES)
            got = from_peer(block, first, at_spot(links, spot), held(local, spot))
            hi, lo = split(jnp.concatenate(turned(got, at_spot(orient, spot, base)), axis=0))
            rhs_hi[at, cols] = hi
            rhs_lo[at, cols] = lo

    def add_top(wait, top):
        @pl.when(has_prev)
        def _():
            wait()
            rhs_hi[wide:], rhs_lo[wide:] = split(top[...])

    def take_in(n):
        near(n).wait_recv()
        add_near(local, links, recv.at[n, 1 - odd], outer + (1 - odd) * peer_tiles)
        add_top(lambda: late(n).wait_recv(), top_recv.at[n])
        pl.when(by_wire(host, n))(lambda: far(n).wait_recv())
        add_far(local, links, orient, 0, recv.at[n, odd], outer + odd * peer_tiles)

    def twin_step(n):
        @pl.when(n == 0)
        def _():
            for part in bulk():
                part.wait_recv()
            twin_state[...] = twin_bias[...] * twin_notes[2 * faces:2 * faces + 1].astype(F32)

        gather_own(twin_state, twin_local, twin_notes)
        feed_twin(n).wait_recv()
        add_near(twin_local, twin_notes, feed.at[n], outer)
        add_top(lambda: tell_twin(n).wait_recv(), twin_top.at[n])
        add_far(twin_local, twin_notes, twin_notes, faces, send.at[n, 0], outer + peer_tiles)
        twin_state[...] = solved(slice(0, size), twin_bias[...], twin_notes[2 * faces:2 * faces + 1].astype(F32))

        @pl.when(n + 1 >= LAG)
        def _():
            for h in range(peer_tiles):
                column = twin_notes[2 * faces + 1:2 * faces + 2, h * LANES:(h + 1) * LANES]
                put(recv.at[n + 1, 0], (0, h), from_state(twin_state, column))

    def solved(at, base, live):
        x_hi, x_lo = rhs_hi[...], rhs_lo[...]
        return (dot(jnp.concatenate([weight_hi[at], weight_lo[at], weight_hi[at]], axis=1), jnp.concatenate([x_hi, x_hi, x_lo], axis=0)) + base) * live

    for load in loads[5:6]:
        load.wait()
    pl.semaphore_wait(barrier, len(peers) + (feeder | teller).astype(jnp.int32))
    send_out(0)
    for load in loads[6:]:
        load.wait()

    @pl.when(home)
    def _():
        notes[:faces] = links[...]
        notes[faces:2 * faces] = orient[...]
        notes[2 * faces:2 * faces + 1] = live.astype(jnp.int32)
        notes[2 * faces + 1:2 * faces + 2, :peer] = exports[1:2]
        notes[2 * faces + 2:] = jnp.zeros((16 - 2 * faces - 2, elems), jnp.int32)
        for part in bulk():
            part.start()

    place = lax.broadcasted_iota(jnp.int32, (wide, wide), 1)
    t, a, b = node_of(place & 63)
    at = (16 * t + 4 * a + b) * faces + (place >> 6)
    order = (at == lax.broadcasted_iota(jnp.int32, (wide, wide), 0)).astype(BF16)
    place = lax.broadcasted_iota(jnp.int32, (FACE, FACE), 1)
    top_order = (point_of(place >> 1, place & 1) == lax.broadcasted_iota(jnp.int32, (FACE, FACE), 0)).astype(BF16)
    lift_hi, lift_lo = split(lift[...])
    lift_hi = jnp.concatenate([dot(lift_hi, order).astype(BF16), dot(lt_hi, top_order).astype(BF16)], axis=1)
    lift_lo = jnp.concatenate([dot(lift_lo, order).astype(BF16), dot(lt_lo, top_order).astype(BF16)], axis=1)
    inv_hi, inv_lo = jnp.concatenate([own_hi, inv_hi], axis=0), jnp.concatenate([own_lo, inv_lo], axis=0)
    part = dot(inv_hi, lift_hi) + dot(inv_lo, lift_hi) + dot(inv_hi, lift_lo)
    weight_hi[...], weight_lo[...] = split(part)
    bias[size:] = dot3(inv_hi[size:], inv_lo[size:], source[0] + dot3(lt_hi, lt_lo, first_top))
    rhs_hi[wide:] = jnp.zeros((FACE, elems), BF16)
    rhs_lo[wide:] = jnp.zeros((FACE, elems), BF16)

    def step(n, carry):
        gather_own(state, local, links)
        pl.when(host & (n > 0))(lambda: twin_step(n - 1))
        take_in(n)
        state[...] = solved(slice(0, size), bias[:size], live)
        send_out(n + 1)
        return carry

    lax.fori_loop(0, hops - 1, step, 0)
    gather_own(state, local, links)
    pl.when(host)(lambda: twin_step(hops - 2))
    take_in(hops - 1)
    out[0] = solved(slice(size, 2 * size), bias[size:], live)

    def sent(n, carry):
        pl.when(by_wire(home, n))(lambda: far(n).wait_send())
        near(n).wait_send()
        pl.when(feeder & (n < hops - 1))(lambda: feed_twin(n).wait_send())
        pl.when(has_next)(lambda: late(n).wait_send())
        pl.when(teller & (n < hops - 1))(lambda: tell_twin(n).wait_send())
        return carry

    lax.fori_loop(0, hops, sent, 0)

    @pl.when(home)
    def _():
        for part in bulk():
            part.wait_send()


def body(n_space, n_slab, source, initial, inverse, lift, lift_time, links, orient, exports, counts):
    size, elems = source.shape[1:]
    wide = links.shape[0] * FACE
    depth = wide + FACE
    peer = exports.shape[0] // 2
    hops = ITERS - 1
    operands = (source, initial, inverse, lift, lift_time.T, links, orient, exports.reshape(2, peer), counts)
    return pl.pallas_call(
        functools.partial(kernel, n_space, n_slab),
        out_shape=pltpu.VMEM(source.shape, F32),
        in_specs=[pl.BlockSpec(memory_space=pltpu.HBM)] * 9,
        out_specs=pl.BlockSpec(memory_space=pltpu.VMEM),
        scratch_shapes=[
            *(pltpu.VMEM(x.shape, x.dtype) for x in operands[:8]),
            pltpu.SMEM(counts.shape, counts.dtype),
            pltpu.SemaphoreType.DMA((9,)),
            pltpu.VMEM((2 * size, depth), BF16),
            pltpu.VMEM((2 * size, depth), BF16),
            pltpu.VMEM((2 * size, elems), F32),
            pltpu.VMEM((depth, elems), BF16),
            pltpu.VMEM((depth, elems), BF16),
            pltpu.VMEM((size, elems), F32),
            pltpu.VMEM((wide, elems), F32),
            pltpu.VMEM((hops, 2, FACE, peer), F32),
            pltpu.VMEM((hops, FACE, elems), F32),
            pltpu.VMEM((hops, 2, FACE, peer), F32),
            pltpu.VMEM((hops, FACE, elems), F32),
            pltpu.SemaphoreType.DMA((hops, 5)),
            pltpu.SemaphoreType.DMA((hops, 5)),
            pltpu.VMEM((16, elems), jnp.int32),
            pltpu.VMEM((16, elems), jnp.int32),
            pltpu.VMEM((size, elems), F32),
            pltpu.VMEM((size, elems), F32),
            pltpu.VMEM((wide, elems), F32),
            pltpu.VMEM((hops, FACE, peer), F32),
            pltpu.VMEM((hops, FACE, elems), F32),
            pltpu.SemaphoreType.DMA((2,)),
            pltpu.SemaphoreType.DMA((2,)),
        ],
        compiler_params=pltpu.CompilerParams(collective_id=0, has_side_effects=True, vmem_limit_bytes=60000 * 1024),
    )(*operands)


def solution(mesh):
    return jax.shard_map(
        functools.partial(body, mesh.shape["space"], mesh.shape["slab"]),
        mesh=mesh,
        in_specs=(
            P("slab", None, "space"),
            P(None, "space"),
            P(),
            P(),
            P(),
            P(None, "space"),
            P(None, "space"),
            P("space"),
            P("space"),
        ),
        out_specs=P("slab", None, "space"),
        check_vma=False,
    )
```

```python
import functools

import jax
import jax.numpy as jnp
from jax import lax
from jax.experimental import pallas as pl
from jax.experimental.pallas import tpu as pltpu
from jax.sharding import PartitionSpec as P

ITERS = 6
LANES = 128
FACE = 64
BY_MATMUL = 6
LAG = 1
F32, BF16 = jnp.float32, jnp.bfloat16
MESH = pl.DeviceIdType.MESH


def split(x):
    hi = x.astype(BF16)
    return hi, (x - hi.astype(F32)).astype(BF16)


def dot(a, b):
    return jnp.dot(a, b, preferred_element_type=F32)


def dot3(ah, al, b):
    bh, bl = split(b)
    return dot(ah, bh) + dot(al, bh) + dot(ah, bl)


def fold(c):
    return (c >> 1) ^ (c & 1)


def node_of(c):
    odd, t, b0, a0, flip = c & 1, (c >> 1) & 3, (c >> 3) & 1, (c >> 4) & 1, (c >> 5) & 1
    return t, 2 * (odd ^ flip ^ a0) + a0, 2 * (flip ^ b0) + b0


def point_of(group, odd):
    k, j, i0 = group & 3, (group >> 2) & 3, group >> 4
    return 16 * (2 * (odd ^ fold(j) ^ fold(k) ^ i0) + i0) + 4 * j + k


def kernel(
    n_space, n_slab,
    source_hbm, initial_hbm, inverse_hbm, lift_hbm, lift_time_hbm, links_hbm, orient_hbm, exports_hbm, out,
    source, initial, inverse, lift, lift_time, links, orient, exports, load_sem,
    weight_hi, weight_lo, bias, rhs_hi, rhs_lo, state, local, send, top_send, recv, top_recv, send_sem, recv_sem,
    hot, twin_hot, notes, twin_notes, twin_bias, twin_state, feed, twin_top, bulk_send, bulk_recv, ready,
):
    size, elems = source.shape[1:]
    faces = links.shape[0]
    wide = faces * FACE
    peer = exports.shape[1]
    tiles, peer_tiles = elems // LANES, peer // LANES
    hops = ITERS - 1

    space, slab = lax.axis_index("space"), lax.axis_index("slab")
    upper, lower = lax.rem(space + 1, n_space), lax.rem(space + n_space - 1, n_space)
    odd = lax.rem(space, 2)
    has_prev, has_next = slab > 0, slab < n_slab - 1
    even, edge = lax.rem(slab, 2) == 0, space == n_space - 1
    host, home = even & (space == 0), even & edge
    feeder, teller = even & (space == n_space - 2), ~even & edge & has_next
    near_first = even & (space < 2)

    barrier = pltpu.get_barrier_semaphore()
    before, after = lax.rem(slab + n_slab - 1, n_slab), lax.rem(slab + 1, n_slab)
    peers = ((lower, slab), (upper, slab), (space, before), (space, after))
    for k, device in enumerate(peers):
        def greet(device=device):
            pl.semaphore_signal(barrier, inc=1, device_id=device, device_id_type=MESH)

        pl.when(~edge)(greet) if k == 1 else greet()

    @pl.when(host)
    def _():
        pl.semaphore_signal(barrier, inc=1, device_id=(n_space - 2, slab), device_id_type=MESH)

    @pl.when(host & has_prev)
    def _():
        pl.semaphore_signal(barrier, inc=1, device_id=(n_space - 1, before), device_id_type=MESH)

    pairs = (
        (inverse_hbm, inverse), (source_hbm, source), (lift_time_hbm, lift_time), (initial_hbm, initial),
        (exports_hbm, exports), (links_hbm, links), (lift_hbm, lift), (orient_hbm, orient),
    )
    loads = [pltpu.make_async_copy(src, dst, load_sem.at[k]) for k, (src, dst) in enumerate(pairs)]
    for load in loads:
        load.start()

    row = lax.broadcasted_iota(jnp.int32, (size, size), 0)
    at = 64 * ((row >> 1) & 3) + point_of(row >> 3, row & 1)
    pick = (at == lax.broadcasted_iota(jnp.int32, (size, size), 1)).astype(BF16)
    for load in loads[:4]:
        load.wait()
    inv_hi, inv_lo = split(inverse[...])
    own_hi, own_lo = dot(pick, inv_hi).astype(BF16), dot(pick, inv_lo).astype(BF16)
    first_top = jnp.where(slab == 0, initial[...], 0.0)
    lt_hi, lt_lo = split(lift_time[...].T)
    top_hi, top_lo = split(first_top)
    lt_wide = jnp.concatenate([lt_hi, lt_lo, lt_hi], axis=1)
    total = source[0] + dot(lt_wide, jnp.concatenate([top_hi, top_hi, top_lo], axis=0))
    rhs_hi[:size], rhs_lo[:size] = split(total)
    first = dot3(own_hi, own_lo, total)
    bias[:size] = first
    state[...] = first

    def copy(src, dst, sems, at, device):
        return pltpu.make_async_remote_copy(
            src_ref=src, dst_ref=dst, send_sem=sems[0].at[at], recv_sem=sems[1].at[at],
            device_id=device, device_id_type=MESH,
        )

    sems, bulk_sems = (send_sem, recv_sem), (bulk_send, bulk_recv)

    def far(n):
        return copy(send.at[n, odd], recv.at[n, 1 - odd], sems, (n, 0), (jnp.where(odd == 1, upper, lower), slab))

    def near(n):
        return copy(send.at[n, 1 - odd], recv.at[n, odd], sems, (n, 1), (jnp.where(odd == 1, lower, upper), slab))

    def late(n):
        return copy(top_send.at[n], top_recv.at[n], sems, (n, 2), (space, after))

    def feed_twin(n):
        return copy(send.at[n, 1 - odd], feed.at[n], sems, (n, 3), (0, slab))

    def tell_twin(n):
        return copy(top_send.at[n], twin_top.at[n], sems, (n, 4), (0, after))

    def bulk():
        return [copy(x, y, bulk_sems, k, (0, slab)) for k, (x, y) in enumerate(((notes, twin_notes), (bias.at[:size], twin_bias)))]

    def spread(column):
        column = jnp.broadcast_to(column, (8, LANES))
        return column & (LANES - 1), column >> 7

    def taken(x, lane):
        return jnp.take_along_axis(x, lane, axis=1, mode="promise_in_bounds")

    def from_state(state, column):
        lane, tile = spread(column)
        face, part = lax.div(tile, tiles), lax.rem(tile, tiles)
        parts = [part == h for h in range(1, tiles)]
        groups = []
        for v in range(size // 8):
            got = taken(state[8 * v:8 * v + 8, :LANES], lane)
            for h in range(1, tiles):
                got = jnp.where(parts[h - 1], taken(state[8 * v:8 * v + 8, h * LANES:(h + 1) * LANES], lane), got)
            groups.append(got)
        return faced(groups, face)

    def faced(groups, face):
        at_face = [face == f for f in range(1, faces)]
        row_odd = (lax.broadcasted_iota(jnp.int32, (8, LANES), 0) & 1) > 0

        def group(i0, j, k):
            return groups[16 * i0 + 4 * j + k]

        result = []
        for q in range(8):
            flip, a0, b0 = q >> 2, (q >> 1) & 1, q & 1
            b = 2 * (flip ^ b0) + b0
            low, high = 2 * (flip ^ a0) + a0, 2 * (1 ^ flip ^ a0) + a0
            sides = [jnp.where(row_odd, group(i0, high, b), group(i0, low, b)) for i0 in range(2)]
            sides += [group(a0, 0, b), group(a0, 3, b), group(a0, b, 0), group(a0, b, 3)]
            x = sides[0]
            for f in range(1, faces):
                x = jnp.where(at_face[f - 1], sides[f], x)
            result.append(x)
        return result

    def from_peer(block, first, column, held):
        lane, tile = spread(column)
        result = held
        for h in range(peer_tiles):
            here = tile == first + h
            result = [
                jnp.where(here, taken(block[8 * q:8 * q + 8, h * LANES:(h + 1) * LANES], lane), result[q])
                for q in range(8)
            ]
        return result

    def turned(groups, code):
        code = jnp.broadcast_to(code, groups[0].shape)
        odd = (lax.broadcasted_iota(jnp.int32, code.shape, 0) & 1) > 0
        swap, back_a, back_b = (code & 4) > 0, (code & 1) > 0, (code & 2) > 0
        swap_odd, swap_even = swap & odd, swap & ~odd
        mid = []
        for q in range(8):
            flip, a0, b0 = q >> 2, (q >> 1) & 1, q & 1
            even_at, odd_at = flip * 4 + b0 * 2 + a0, (1 - flip) * 4 + b0 * 2 + a0
            mid.append(jnp.where(swap_odd, groups[odd_at], jnp.where(swap_even, groups[even_at], groups[q])))
        mid = [jnp.where(back_a, mid[q ^ 2], mid[q]) for q in range(8)]
        return [jnp.where(back_b, mid[q ^ 1], mid[q]) for q in range(8)]

    def put(ref, spot, groups):
        f, h = spot
        for q in range(8):
            ref[f * FACE + 8 * q:f * FACE + 8 * q + 8, h * LANES:(h + 1) * LANES] = groups[q]

    def held(ref, spot):
        f, h = spot
        return [ref[f * FACE + 8 * q:f * FACE + 8 * q + 8, h * LANES:(h + 1) * LANES] for q in range(8)]

    def at_spot(ref, spot, base=0):
        f, h = spot
        return ref[base + f:base + f + 1, h * LANES:(h + 1) * LANES]

    spots = [(f, h) for f in range(faces) for h in range(tiles)]
    outer = faces * tiles

    def pack_top(state, dst):
        sub = lax.broadcasted_iota(jnp.int32, (8, elems), 0) >> 1
        for w in range(8):
            pack = state[32 * w + 24:32 * w + 32]
            for m in range(3):
                pack = jnp.where(sub == m, pltpu.roll(state[32 * w + 8 * m:32 * w + 8 * m + 8], 2 * m + 2, 0), pack)
            dst[8 * w:8 * w + 8] = pack

    def by_wire(edge_kind, n):
        return jnp.logical_or(jnp.logical_not(edge_kind), n < LAG)

    def send_out(n, far_now=True):
        def start_near():
            near(n).start()
            pl.when(feeder & (n < hops - 1))(lambda: feed_twin(n).start())

        ahead = jnp.where(near_first, 1 - odd, odd)
        for half, is_near in ((ahead, near_first), (1 - ahead, ~near_first)):
            for h in range(peer_tiles):
                cols = slice(h * LANES, (h + 1) * LANES)
                put(send.at[n, half], (0, h), from_state(state, exports[pl.ds(half, 1), cols]))
            pl.when(is_near)(start_near)
            pl.when(~is_near & by_wire(home, n) & far_now)(lambda: far(n).start())
        pack_top(state, top_send.at[n])
        pl.when(has_next)(lambda: late(n).start())
        pl.when(teller & (n < hops - 1))(lambda: tell_twin(n).start())

    def one_hot(links, hot):
        element = lax.broadcasted_iota(jnp.int32, (elems, LANES), 0)
        for f, h in spots:
            if f < BY_MATMUL:
                column = lax.rem(at_spot(links, (f, h)), elems)
                cols = slice(f * elems + h * LANES, f * elems + (h + 1) * LANES)
                hot[:, cols] = (element == column).astype(F32).astype(BF16)

    def gather_own(state, local, links, hot):
        hi, lo = split(state[...])
        for f in range(faces):
            if f < BY_MATMUL:
                eye = hot[:, f * elems:(f + 1) * elems]
                got = dot(hi, eye) + dot(lo, eye)
                for h in range(tiles):
                    groups = [got[8 * v:8 * v + 8, h * LANES:(h + 1) * LANES] for v in range(size // 8)]
                    put(local, (f, h), faced(groups, lax.div(spread(at_spot(links, (f, h)))[1], tiles)))
            else:
                for h in range(tiles):
                    put(local, (f, h), from_state(state, at_spot(links, (f, h))))

    def add_near(local, links, block, first):
        for spot in spots:
            put(local, spot, from_peer(block, first, at_spot(links, spot), held(local, spot)))

    def turned_in(spot, groups):
        f, h = spot
        at, cols = slice(f * FACE, (f + 1) * FACE), slice(h * LANES, (h + 1) * LANES)
        rhs_hi[at, cols], rhs_lo[at, cols] = split(jnp.concatenate(groups, axis=0))

    def add_far(local, links, orient, base, block, first):
        for spot in spots:
            got = from_peer(block, first, at_spot(links, spot), held(local, spot))
            turned_in(spot, turned(got, at_spot(orient, spot, base)))

    def add_top(wait, top):
        @pl.when(has_prev)
        def _():
            wait()
            rhs_hi[wide:], rhs_lo[wide:] = split(top[...])

    def take_in(n):
        def wait(is_near):
            pl.when(is_near)(lambda: near(n).wait_recv())
            pl.when(~is_near & by_wire(host, n))(lambda: far(n).wait_recv())

        near_last = near_first & ((space > 0) | (n >= LAG))
        first_side = jnp.where(near_last, odd, 1 - odd)
        wait(~near_last)
        add_near(local, links, recv.at[n, first_side], outer + first_side * peer_tiles)
        add_top(lambda: late(n).wait_recv(), top_recv.at[n])
        wait(near_last)
        add_far(local, links, orient, 0, recv.at[n, 1 - first_side], outer + (1 - first_side) * peer_tiles)

    def twin_step(n):
        @pl.when(n == 0)
        def _():
            told, biases = bulk()
            told.wait_recv()
            one_hot(twin_notes, twin_hot)
            biases.wait_recv()
            twin_state[...] = twin_bias[...]

        feed_twin(n).wait_recv()
        add_top(lambda: tell_twin(n).wait_recv(), twin_top.at[n])
        hi, lo = split(twin_state[...])
        for f in range(faces):
            if f < BY_MATMUL:
                eye = twin_hot[:, f * elems:(f + 1) * elems]
                got = dot(hi, eye) + dot(lo, eye)
            for h in range(tiles):
                spot = (f, h)
                column = at_spot(twin_notes, spot)
                if f < BY_MATMUL:
                    groups = [got[8 * v:8 * v + 8, h * LANES:(h + 1) * LANES] for v in range(size // 8)]
                    groups = faced(groups, lax.div(spread(column)[1], tiles))
                else:
                    groups = from_state(twin_state, column)
                groups = from_peer(feed.at[n], outer, column, groups)
                groups = from_peer(send.at[n, 0], outer + peer_tiles, column, groups)
                turned_in(spot, turned(groups, at_spot(twin_notes, spot, faces)))
        twin_state[...] = solved(slice(0, size), twin_bias[...])

        @pl.when(n + 1 >= LAG)
        def _():
            for h in range(peer_tiles):
                column = twin_notes[2 * faces:2 * faces + 1, h * LANES:(h + 1) * LANES]
                put(recv.at[n + 1, 0], (0, h), from_state(twin_state, column))

    def solved(at, base):
        x_hi, x_lo = rhs_hi[...], rhs_lo[...]
        return dot(jnp.concatenate([weight_hi[at], weight_lo[at], weight_hi[at]], axis=1), jnp.concatenate([x_hi, x_hi, x_lo], axis=0)) + base

    for load in loads[4:5]:
        load.wait()
    pl.semaphore_wait(barrier, len(peers) + (feeder | teller).astype(jnp.int32) - (space == 0).astype(jnp.int32))

    @pl.when(edge)
    def _():
        pl.semaphore_signal(ready, inc=1, device_id=(0, slab), device_id_type=MESH)

    send_out(0, space > 0)
    for load in loads[5:]:
        load.wait()
    one_hot(links, hot)

    @pl.when(home)
    def _():
        notes[:faces] = links[...]
        notes[faces:2 * faces] = orient[...]
        notes[2 * faces:] = jnp.zeros((16 - 2 * faces, elems), jnp.int32)
        notes[2 * faces:2 * faces + 1, :peer] = exports[1:2]
        for part in bulk():
            part.start()

    place = lax.broadcasted_iota(jnp.int32, (wide, wide), 1)
    t, a, b = node_of(place & 63)
    at = (16 * t + 4 * a + b) * faces + (place >> 6)
    order = (at == lax.broadcasted_iota(jnp.int32, (wide, wide), 0)).astype(BF16)
    place = lax.broadcasted_iota(jnp.int32, (FACE, FACE), 1)
    top_order = (point_of(place >> 1, place & 1) == lax.broadcasted_iota(jnp.int32, (FACE, FACE), 0)).astype(BF16)
    lift_hi, lift_lo = split(lift[...])
    lift_hi = jnp.concatenate([dot(lift_hi, order).astype(BF16), dot(lt_hi, top_order).astype(BF16)], axis=1)
    lift_lo = jnp.concatenate([dot(lift_lo, order).astype(BF16), dot(lt_lo, top_order).astype(BF16)], axis=1)
    inv_hi, inv_lo = jnp.concatenate([own_hi, inv_hi], axis=0), jnp.concatenate([own_lo, inv_lo], axis=0)
    part = dot(inv_hi, lift_hi) + dot(inv_lo, lift_hi) + dot(inv_hi, lift_lo)
    weight_hi[...], weight_lo[...] = split(part)
    total_hi, total_lo = rhs_hi[:size], rhs_lo[:size]
    bias[size:] = dot(inv_hi[size:], total_hi) + dot(inv_lo[size:], total_hi) + dot(inv_hi[size:], total_lo)
    @pl.when(space == 0)
    def _():
        pl.semaphore_wait(ready, 1)
        far(0).start()

    rhs_hi[wide:] = jnp.zeros((FACE, elems), BF16)
    rhs_lo[wide:] = jnp.zeros((FACE, elems), BF16)

    def step(n, carry):
        gather_own(state, local, links, hot)
        pl.when(host & (n > 0))(lambda: twin_step(n - 1))
        take_in(n)
        state[...] = solved(slice(0, size), bias[:size])
        send_out(n + 1)
        return carry

    lax.fori_loop(0, hops - 1, step, 0)
    gather_own(state, local, links, hot)
    pl.when(host)(lambda: twin_step(hops - 2))
    take_in(hops - 1)
    out[0] = solved(slice(size, 2 * size), bias[size:])

    def sent(n, carry):
        pl.when(by_wire(home, n))(lambda: far(n).wait_send())
        near(n).wait_send()
        pl.when(feeder & (n < hops - 1))(lambda: feed_twin(n).wait_send())
        pl.when(has_next)(lambda: late(n).wait_send())
        pl.when(teller & (n < hops - 1))(lambda: tell_twin(n).wait_send())
        return carry

    lax.fori_loop(0, hops, sent, 0)

    @pl.when(home)
    def _():
        for part in bulk():
            part.wait_send()


def body(n_space, n_slab, source, initial, inverse, lift, lift_time, links, orient, exports, counts):
    size, elems = source.shape[1:]
    wide = links.shape[0] * FACE
    depth = wide + FACE
    peer = exports.shape[0] // 2
    hops = ITERS - 1
    operands = (source, initial, inverse, lift, lift_time.T, links, orient, exports.reshape(2, peer))
    result = pl.pallas_call(
        functools.partial(kernel, n_space, n_slab),
        out_shape=pltpu.VMEM(source.shape, F32),
        in_specs=[pl.BlockSpec(memory_space=pltpu.HBM)] * 8,
        out_specs=pl.BlockSpec(memory_space=pltpu.VMEM),
        scratch_shapes=[
            *(pltpu.VMEM(x.shape, x.dtype) for x in operands),
            pltpu.SemaphoreType.DMA((8,)),
            pltpu.VMEM((2 * size, depth), BF16),
            pltpu.VMEM((2 * size, depth), BF16),
            pltpu.VMEM((2 * size, elems), F32),
            pltpu.VMEM((depth, elems), BF16),
            pltpu.VMEM((depth, elems), BF16),
            pltpu.VMEM((size, elems), F32),
            pltpu.VMEM((wide, elems), F32),
            pltpu.VMEM((hops, 2, FACE, peer), F32),
            pltpu.VMEM((hops, FACE, elems), F32),
            pltpu.VMEM((hops, 2, FACE, peer), F32),
            pltpu.VMEM((hops, FACE, elems), F32),
            pltpu.SemaphoreType.DMA((hops, 5)),
            pltpu.SemaphoreType.DMA((hops, 5)),
            pltpu.VMEM((elems, BY_MATMUL * elems), BF16),
            pltpu.VMEM((elems, BY_MATMUL * elems), BF16),
            pltpu.VMEM((16, elems), jnp.int32),
            pltpu.VMEM((16, elems), jnp.int32),
            pltpu.VMEM((size, elems), F32),
            pltpu.VMEM((size, elems), F32),
            pltpu.VMEM((hops, FACE, peer), F32),
            pltpu.VMEM((hops, FACE, elems), F32),
            pltpu.SemaphoreType.DMA((2,)),
            pltpu.SemaphoreType.DMA((2,)),
            pltpu.SemaphoreType.REGULAR,
        ],
        compiler_params=pltpu.CompilerParams(collective_id=0, has_side_effects=True, vmem_limit_bytes=60000 * 1024),
    )(*operands)
    return jnp.where(lax.broadcasted_iota(jnp.int32, result.shape, 2) < counts.reshape(1, 1, 1), result, 0.0)


def solution(mesh):
    return jax.shard_map(
        functools.partial(body, mesh.shape["space"], mesh.shape["slab"]),
        mesh=mesh,
        in_specs=(
            P("slab", None, "space"),
            P(None, "space"),
            P(),
            P(),
            P(),
            P(None, "space"),
            P(None, "space"),
            P("space"),
            P("space"),
        ),
        out_specs=P("slab", None, "space"),
        check_vma=False,
    )
```

```python
import functools

import jax
import jax.numpy as jnp
from jax import lax
from jax.experimental import pallas as pl
from jax.experimental.pallas import tpu as pltpu
from jax.sharding import PartitionSpec as P

ITERS = 6
LANES = 128
FACE = 64
BY_MATMUL = 6
LAG = 1
F32, BF16 = jnp.float32, jnp.bfloat16
MESH = pl.DeviceIdType.MESH


def split(x):
    hi = x.astype(BF16)
    return hi, (x - hi.astype(F32)).astype(BF16)


def dot(a, b):
    return jnp.dot(a, b, preferred_element_type=F32)


def dot_t(a, b):
    return lax.dot_general(a, b, (((1,), (1,)), ((), ())), preferred_element_type=F32)


def dot3(ah, al, b):
    bh, bl = split(b)
    return dot(ah, bh) + dot(al, bh) + dot(ah, bl)


def fold(c):
    return (c >> 1) ^ (c & 1)


def node_of(c):
    odd, t, b0, a0, flip = c & 1, (c >> 1) & 3, (c >> 3) & 1, (c >> 4) & 1, (c >> 5) & 1
    return t, 2 * (odd ^ flip ^ a0) + a0, 2 * (flip ^ b0) + b0


def point_of(group, odd):
    k, j, i0 = group & 3, (group >> 2) & 3, group >> 4
    return 16 * (2 * (odd ^ fold(j) ^ fold(k) ^ i0) + i0) + 4 * j + k


def kernel(
    n_space, n_slab,
    source_hbm, initial_hbm, inverse_hbm, lift_hbm, lift_time_hbm, links_hbm, orient_hbm, exports_hbm, out,
    source, initial, inverse, lift, lift_time, links, orient, exports, load_sem,
    weight_hi, weight_lo, bias, rhs_hi, rhs_lo, state, local, send, top_send, recv, top_recv, send_sem, recv_sem,
    hot, twin_hot, notes, twin_notes, twin_bias, twin_state, feed, twin_top, bulk_send, bulk_recv, ready,
):
    size, elems = source.shape[1:]
    faces = links.shape[0]
    wide = faces * FACE
    peer = exports.shape[1]
    tiles, peer_tiles = elems // LANES, peer // LANES
    hops = ITERS - 1

    space, slab = lax.axis_index("space"), lax.axis_index("slab")
    upper, lower = lax.rem(space + 1, n_space), lax.rem(space + n_space - 1, n_space)
    odd = lax.rem(space, 2)
    has_prev, has_next = slab > 0, slab < n_slab - 1
    even, edge = lax.rem(slab, 2) == 0, space == n_space - 1
    host, home = even & (space == 0), even & edge
    feeder, teller = even & (space == n_space - 2), ~even & edge & has_next
    near_first = even & (space < 2)

    barrier = pltpu.get_barrier_semaphore()
    before, after = lax.rem(slab + n_slab - 1, n_slab), lax.rem(slab + 1, n_slab)
    peers = ((lower, slab), (upper, slab), (space, before), (space, after))
    for k, device in enumerate(peers):
        def greet(device=device):
            pl.semaphore_signal(barrier, inc=1, device_id=device, device_id_type=MESH)

        pl.when(~edge)(greet) if k == 1 else greet()

    @pl.when(host)
    def _():
        pl.semaphore_signal(barrier, inc=1, device_id=(n_space - 2, slab), device_id_type=MESH)

    @pl.when(host & has_prev)
    def _():
        pl.semaphore_signal(barrier, inc=1, device_id=(n_space - 1, before), device_id_type=MESH)

    pairs = (
        (inverse_hbm, inverse), (source_hbm, source), (lift_time_hbm, lift_time), (initial_hbm, initial),
        (exports_hbm, exports), (links_hbm, links), (lift_hbm, lift), (orient_hbm, orient),
    )
    loads = [pltpu.make_async_copy(src, dst, load_sem.at[k]) for k, (src, dst) in enumerate(pairs)]
    for load in loads:
        load.start()

    row = lax.broadcasted_iota(jnp.int32, (size, size), 0)
    at = 64 * ((row >> 1) & 3) + point_of(row >> 3, row & 1)
    pick = (at == lax.broadcasted_iota(jnp.int32, (size, size), 1)).astype(BF16)
    for load in loads[:4]:
        load.wait()
    inv_hi, inv_lo = split(inverse[...])
    own_hi, own_lo = dot(pick, inv_hi).astype(BF16), dot(pick, inv_lo).astype(BF16)
    first_top = jnp.where(slab == 0, initial[...], 0.0)
    top_hi, top_lo = split(first_top)
    lt_hi, lt_lo = split(jnp.concatenate([lift_time[...]] * 2, axis=0))
    time_part = dot_t(own_hi, lt_hi) + dot_t(own_lo, lt_hi) + dot_t(own_hi, lt_lo)
    time_hi = time_part.astype(BF16).astype(F32)
    left = lax.broadcasted_iota(jnp.int32, time_part.shape, 1) < FACE
    time_wide = jnp.concatenate([jnp.where(left, time_hi, time_part - time_hi), time_hi], axis=1).astype(BF16)
    top_wide = jnp.concatenate([top_hi, top_hi, top_lo, jnp.zeros_like(top_hi)], axis=0)
    first = dot3(own_hi, own_lo, source[0]) + dot(time_wide, top_wide)
    bias[:size] = first
    state[...] = first

    def copy(src, dst, sems, at, device):
        return pltpu.make_async_remote_copy(
            src_ref=src, dst_ref=dst, send_sem=sems[0].at[at], recv_sem=sems[1].at[at],
            device_id=device, device_id_type=MESH,
        )

    sems, bulk_sems = (send_sem, recv_sem), (bulk_send, bulk_recv)

    def far(n):
        return copy(send.at[n, odd], recv.at[n, 1 - odd], sems, (n, 0), (jnp.where(odd == 1, upper, lower), slab))

    def near(n):
        return copy(send.at[n, 1 - odd], recv.at[n, odd], sems, (n, 1), (jnp.where(odd == 1, lower, upper), slab))

    def late(n):
        return copy(top_send.at[n], top_recv.at[n], sems, (n, 2), (space, after))

    def feed_twin(n):
        return copy(send.at[n, 1 - odd], feed.at[n], sems, (n, 3), (0, slab))

    def tell_twin(n):
        return copy(top_send.at[n], twin_top.at[n], sems, (n, 4), (0, after))

    def bulk():
        return [copy(x, y, bulk_sems, k, (0, slab)) for k, (x, y) in enumerate(((notes, twin_notes), (bias.at[:size], twin_bias)))]

    def spread(column):
        column = jnp.broadcast_to(column, (8, LANES))
        return column & (LANES - 1), column >> 7

    def taken(x, lane):
        return jnp.take_along_axis(x, lane, axis=1, mode="promise_in_bounds")

    def from_state(state, column):
        lane, tile = spread(column)
        face, part = lax.div(tile, tiles), lax.rem(tile, tiles)
        parts = [part == h for h in range(1, tiles)]
        groups = []
        for v in range(size // 8):
            got = taken(state[8 * v:8 * v + 8, :LANES], lane)
            for h in range(1, tiles):
                got = jnp.where(parts[h - 1], taken(state[8 * v:8 * v + 8, h * LANES:(h + 1) * LANES], lane), got)
            groups.append(got)
        return faced(groups, face)

    def faced(groups, face):
        at_face = [face == f for f in range(1, faces)]
        row_odd = (lax.broadcasted_iota(jnp.int32, (8, LANES), 0) & 1) > 0

        def group(i0, j, k):
            return groups[16 * i0 + 4 * j + k]

        result = []
        for q in range(8):
            flip, a0, b0 = q >> 2, (q >> 1) & 1, q & 1
            b = 2 * (flip ^ b0) + b0
            low, high = 2 * (flip ^ a0) + a0, 2 * (1 ^ flip ^ a0) + a0
            sides = [jnp.where(row_odd, group(i0, high, b), group(i0, low, b)) for i0 in range(2)]
            sides += [group(a0, 0, b), group(a0, 3, b), group(a0, b, 0), group(a0, b, 3)]
            x = sides[0]
            for f in range(1, faces):
                x = jnp.where(at_face[f - 1], sides[f], x)
            result.append(x)
        return result

    def from_peer(block, first, column, held):
        lane, tile = spread(column)
        result = held
        for h in range(peer_tiles):
            here = tile == first + h
            result = [
                jnp.where(here, taken(block[8 * q:8 * q + 8, h * LANES:(h + 1) * LANES], lane), result[q])
                for q in range(8)
            ]
        return result

    def turned(groups, code):
        code = jnp.broadcast_to(code, groups[0].shape)
        odd = (lax.broadcasted_iota(jnp.int32, code.shape, 0) & 1) > 0
        swap, back_a, back_b = (code & 4) > 0, (code & 1) > 0, (code & 2) > 0
        swap_odd, swap_even = swap & odd, swap & ~odd
        mid = []
        for q in range(8):
            flip, a0, b0 = q >> 2, (q >> 1) & 1, q & 1
            even_at, odd_at = flip * 4 + b0 * 2 + a0, (1 - flip) * 4 + b0 * 2 + a0
            mid.append(jnp.where(swap_odd, groups[odd_at], jnp.where(swap_even, groups[even_at], groups[q])))
        mid = [jnp.where(back_a, mid[q ^ 2], mid[q]) for q in range(8)]
        return [jnp.where(back_b, mid[q ^ 1], mid[q]) for q in range(8)]

    def put(ref, spot, groups):
        f, h = spot
        for q in range(8):
            ref[f * FACE + 8 * q:f * FACE + 8 * q + 8, h * LANES:(h + 1) * LANES] = groups[q]

    def held(ref, spot):
        f, h = spot
        return [ref[f * FACE + 8 * q:f * FACE + 8 * q + 8, h * LANES:(h + 1) * LANES] for q in range(8)]

    def at_spot(ref, spot, base=0):
        f, h = spot
        return ref[base + f:base + f + 1, h * LANES:(h + 1) * LANES]

    spots = [(f, h) for f in range(faces) for h in range(tiles)]
    outer = faces * tiles

    def pack_top(state, dst):
        sub = lax.broadcasted_iota(jnp.int32, (8, elems), 0) >> 1
        for w in range(8):
            pack = state[32 * w + 24:32 * w + 32]
            for m in range(3):
                pack = jnp.where(sub == m, pltpu.roll(state[32 * w + 8 * m:32 * w + 8 * m + 8], 2 * m + 2, 0), pack)
            dst[8 * w:8 * w + 8] = pack

    def by_wire(edge_kind, n):
        return jnp.logical_or(jnp.logical_not(edge_kind), n < LAG)

    def send_out(n, far_now=True):
        def start_near():
            near(n).start()
            pl.when(feeder & (n < hops - 1))(lambda: feed_twin(n).start())

        ahead = jnp.where(near_first, 1 - odd, odd)
        for half, is_near in ((ahead, near_first), (1 - ahead, ~near_first)):
            for h in range(peer_tiles):
                cols = slice(h * LANES, (h + 1) * LANES)
                put(send.at[n, half], (0, h), from_state(state, exports[pl.ds(half, 1), cols]))
            pl.when(is_near)(start_near)
            pl.when(~is_near & by_wire(home, n) & far_now)(lambda: far(n).start())
        pack_top(state, top_send.at[n])
        pl.when(has_next)(lambda: late(n).start())
        pl.when(teller & (n < hops - 1))(lambda: tell_twin(n).start())

    def one_hot(links, hot):
        element = lax.broadcasted_iota(jnp.int32, (elems, LANES), 0)
        for f, h in spots:
            if f < BY_MATMUL:
                column = lax.rem(at_spot(links, (f, h)), elems)
                cols = slice(f * elems + h * LANES, f * elems + (h + 1) * LANES)
                hot[:, cols] = (element == column).astype(F32).astype(BF16)

    def gather_own(state, local, links, hot):
        hi, lo = split(state[...])
        for f in range(faces):
            if f < BY_MATMUL:
                eye = hot[:, f * elems:(f + 1) * elems]
                got = dot(hi, eye) + dot(lo, eye)
                for h in range(tiles):
                    groups = [got[8 * v:8 * v + 8, h * LANES:(h + 1) * LANES] for v in range(size // 8)]
                    put(local, (f, h), faced(groups, lax.div(spread(at_spot(links, (f, h)))[1], tiles)))
            else:
                for h in range(tiles):
                    put(local, (f, h), from_state(state, at_spot(links, (f, h))))

    def add_near(local, links, block, first):
        for spot in spots:
            put(local, spot, from_peer(block, first, at_spot(links, spot), held(local, spot)))

    def turned_in(spot, groups):
        f, h = spot
        at, cols = slice(f * FACE, (f + 1) * FACE), slice(h * LANES, (h + 1) * LANES)
        rhs_hi[at, cols], rhs_lo[at, cols] = split(jnp.concatenate(groups, axis=0))

    def add_far(local, links, orient, base, block, first):
        for spot in spots:
            got = from_peer(block, first, at_spot(links, spot), held(local, spot))
            turned_in(spot, turned(got, at_spot(orient, spot, base)))

    def add_top(wait, top):
        @pl.when(has_prev)
        def _():
            wait()
            rhs_hi[wide:], rhs_lo[wide:] = split(top[...])

    def take_in(n):
        def wait(is_near):
            pl.when(is_near)(lambda: near(n).wait_recv())
            pl.when(~is_near & by_wire(host, n))(lambda: far(n).wait_recv())

        near_last = near_first & ((space > 0) | (n >= LAG))
        first_side = jnp.where(near_last, odd, 1 - odd)
        wait(~near_last)
        add_near(local, links, recv.at[n, first_side], outer + first_side * peer_tiles)
        add_top(lambda: late(n).wait_recv(), top_recv.at[n])
        wait(near_last)
        add_far(local, links, orient, 0, recv.at[n, 1 - first_side], outer + (1 - first_side) * peer_tiles)

    def twin_step(n):
        @pl.when(n == 0)
        def _():
            told, biases = bulk()
            told.wait_recv()
            one_hot(twin_notes, twin_hot)
            biases.wait_recv()
            twin_state[...] = twin_bias[...]

        feed_twin(n).wait_recv()
        add_top(lambda: tell_twin(n).wait_recv(), twin_top.at[n])
        hi, lo = split(twin_state[...])
        for f in range(faces):
            if f < BY_MATMUL:
                eye = twin_hot[:, f * elems:(f + 1) * elems]
                got = dot(hi, eye) + dot(lo, eye)
            for h in range(tiles):
                spot = (f, h)
                column = at_spot(twin_notes, spot)
                if f < BY_MATMUL:
                    groups = [got[8 * v:8 * v + 8, h * LANES:(h + 1) * LANES] for v in range(size // 8)]
                    groups = faced(groups, lax.div(spread(column)[1], tiles))
                else:
                    groups = from_state(twin_state, column)
                groups = from_peer(feed.at[n], outer, column, groups)
                groups = from_peer(send.at[n, 0], outer + peer_tiles, column, groups)
                turned_in(spot, turned(groups, at_spot(twin_notes, spot, faces)))
        twin_state[...] = solved(slice(0, size), twin_bias[...])

        @pl.when(n + 1 >= LAG)
        def _():
            for h in range(peer_tiles):
                column = twin_notes[2 * faces:2 * faces + 1, h * LANES:(h + 1) * LANES]
                put(recv.at[n + 1, 0], (0, h), from_state(twin_state, column))

    def solved(at, base):
        x_hi, x_lo = rhs_hi[...], rhs_lo[...]
        return dot(jnp.concatenate([weight_hi[at], weight_lo[at], weight_hi[at]], axis=1), jnp.concatenate([x_hi, x_hi, x_lo], axis=0)) + base

    for load in loads[4:5]:
        load.wait()
    pl.semaphore_wait(barrier, len(peers) + (feeder | teller).astype(jnp.int32) - (space == 0).astype(jnp.int32))

    @pl.when(edge)
    def _():
        pl.semaphore_signal(ready, inc=1, device_id=(0, slab), device_id_type=MESH)

    send_out(0, space > 0)
    for load in loads[5:]:
        load.wait()
    one_hot(links, hot)

    @pl.when(home)
    def _():
        notes[:faces] = links[...]
        notes[faces:2 * faces] = orient[...]
        notes[2 * faces:] = jnp.zeros((16 - 2 * faces, elems), jnp.int32)
        notes[2 * faces:2 * faces + 1, :peer] = exports[1:2]
        for part in bulk():
            part.start()

    place = lax.broadcasted_iota(jnp.int32, (wide, wide), 1)
    t, a, b = node_of(place & 63)
    at = (16 * t + 4 * a + b) * faces + (place >> 6)
    order = (at == lax.broadcasted_iota(jnp.int32, (wide, wide), 0)).astype(BF16)
    place = lax.broadcasted_iota(jnp.int32, (FACE, FACE), 1)
    top_order = (point_of(place >> 1, place & 1) == lax.broadcasted_iota(jnp.int32, (FACE, FACE), 0)).astype(BF16)
    lt_hi, lt_lo = split(lift_time[...].T)
    lt_wide = jnp.concatenate([lt_hi, lt_lo, lt_hi], axis=1)
    total_hi, total_lo = split(source[0] + dot(lt_wide, jnp.concatenate([top_hi, top_hi, top_lo], axis=0)))
    lift_hi, lift_lo = split(lift[...])
    lift_hi = jnp.concatenate([dot(lift_hi, order).astype(BF16), dot(lt_hi, top_order).astype(BF16)], axis=1)
    lift_lo = jnp.concatenate([dot(lift_lo, order).astype(BF16), dot(lt_lo, top_order).astype(BF16)], axis=1)
    inv_hi, inv_lo = jnp.concatenate([own_hi, inv_hi], axis=0), jnp.concatenate([own_lo, inv_lo], axis=0)
    part = dot(inv_hi, lift_hi) + dot(inv_lo, lift_hi) + dot(inv_hi, lift_lo)
    weight_hi[...], weight_lo[...] = split(part)
    bias[size:] = dot(inv_hi[size:], total_hi) + dot(inv_lo[size:], total_hi) + dot(inv_hi[size:], total_lo)
    @pl.when(space == 0)
    def _():
        pl.semaphore_wait(ready, 1)
        far(0).start()

    rhs_hi[wide:] = jnp.zeros((FACE, elems), BF16)
    rhs_lo[wide:] = jnp.zeros((FACE, elems), BF16)

    def step(n, carry):
        gather_own(state, local, links, hot)
        pl.when(host & (n > 0))(lambda: twin_step(n - 1))
        take_in(n)
        state[...] = solved(slice(0, size), bias[:size])
        send_out(n + 1)
        return carry

    lax.fori_loop(0, hops - 1, step, 0)
    gather_own(state, local, links, hot)
    pl.when(host)(lambda: twin_step(hops - 2))
    take_in(hops - 1)
    out[0] = solved(slice(size, 2 * size), bias[size:])

    def sent(n, carry):
        pl.when(by_wire(home, n))(lambda: far(n).wait_send())
        near(n).wait_send()
        pl.when(feeder & (n < hops - 1))(lambda: feed_twin(n).wait_send())
        pl.when(has_next)(lambda: late(n).wait_send())
        pl.when(teller & (n < hops - 1))(lambda: tell_twin(n).wait_send())
        return carry

    lax.fori_loop(0, hops, sent, 0)

    @pl.when(home)
    def _():
        for part in bulk():
            part.wait_send()


def body(n_space, n_slab, source, initial, inverse, lift, lift_time, links, orient, exports, counts):
    size, elems = source.shape[1:]
    wide = links.shape[0] * FACE
    depth = wide + FACE
    peer = exports.shape[0] // 2
    hops = ITERS - 1
    operands = (source, initial, inverse, lift, lift_time.T, links, orient, exports.reshape(2, peer))
    result = pl.pallas_call(
        functools.partial(kernel, n_space, n_slab),
        out_shape=pltpu.VMEM(source.shape, F32),
        in_specs=[pl.BlockSpec(memory_space=pltpu.HBM)] * 8,
        out_specs=pl.BlockSpec(memory_space=pltpu.VMEM),
        scratch_shapes=[
            *(pltpu.VMEM(x.shape, x.dtype) for x in operands),
            pltpu.SemaphoreType.DMA((8,)),
            pltpu.VMEM((2 * size, depth), BF16),
            pltpu.VMEM((2 * size, depth), BF16),
            pltpu.VMEM((2 * size, elems), F32),
            pltpu.VMEM((depth, elems), BF16),
            pltpu.VMEM((depth, elems), BF16),
            pltpu.VMEM((size, elems), F32),
            pltpu.VMEM((wide, elems), F32),
            pltpu.VMEM((hops, 2, FACE, peer), F32),
            pltpu.VMEM((hops, FACE, elems), F32),
            pltpu.VMEM((hops, 2, FACE, peer), F32),
            pltpu.VMEM((hops, FACE, elems), F32),
            pltpu.SemaphoreType.DMA((hops, 5)),
            pltpu.SemaphoreType.DMA((hops, 5)),
            pltpu.VMEM((elems, BY_MATMUL * elems), BF16),
            pltpu.VMEM((elems, BY_MATMUL * elems), BF16),
            pltpu.VMEM((16, elems), jnp.int32),
            pltpu.VMEM((16, elems), jnp.int32),
            pltpu.VMEM((size, elems), F32),
            pltpu.VMEM((size, elems), F32),
            pltpu.VMEM((hops, FACE, peer), F32),
            pltpu.VMEM((hops, FACE, elems), F32),
            pltpu.SemaphoreType.DMA((2,)),
            pltpu.SemaphoreType.DMA((2,)),
            pltpu.SemaphoreType.REGULAR,
        ],
        compiler_params=pltpu.CompilerParams(collective_id=0, has_side_effects=True, vmem_limit_bytes=60000 * 1024),
    )(*operands)
    return jnp.where(lax.broadcasted_iota(jnp.int32, result.shape, 2) < counts.reshape(1, 1, 1), result, 0.0)


def solution(mesh):
    return jax.shard_map(
        functools.partial(body, mesh.shape["space"], mesh.shape["slab"]),
        mesh=mesh,
        in_specs=(
            P("slab", None, "space"),
            P(None, "space"),
            P(),
            P(),
            P(),
            P(None, "space"),
            P(None, "space"),
            P("space"),
            P("space"),
        ),
        out_specs=P("slab", None, "space"),
        check_vma=False,
    )
```

```python
import functools

import jax
import jax.numpy as jnp
from jax import lax
from jax.experimental import pallas as pl
from jax.experimental.pallas import tpu as pltpu
from jax.sharding import PartitionSpec as P

ITERS = 6
LANES = 128
FACE = 64
BY_MATMUL = 6
LAG = 1
F32, BF16 = jnp.float32, jnp.bfloat16
MESH = pl.DeviceIdType.MESH


def split(x):
    hi = x.astype(BF16)
    return hi, (x - hi.astype(F32)).astype(BF16)


def dot(a, b):
    return jnp.dot(a, b, preferred_element_type=F32)


def dot_t(a, b):
    return lax.dot_general(a, b, (((1,), (1,)), ((), ())), preferred_element_type=F32)


def dot3(ah, al, b):
    bh, bl = split(b)
    return dot(ah, bh) + dot(al, bh) + dot(ah, bl)


def fold(c):
    return (c >> 1) ^ (c & 1)


def node_of(c):
    odd, t, b0, a0, flip = c & 1, (c >> 1) & 3, (c >> 3) & 1, (c >> 4) & 1, (c >> 5) & 1
    return t, 2 * (odd ^ flip ^ a0) + a0, 2 * (flip ^ b0) + b0


def point_of(group, odd):
    k, j, i0 = group & 3, (group >> 2) & 3, group >> 4
    return 16 * (2 * (odd ^ fold(j) ^ fold(k) ^ i0) + i0) + 4 * j + k


def kernel(
    n_space, n_slab,
    source_hbm, initial_hbm, inverse_hbm, lift_hbm, lift_time_hbm, links_hbm, orient_hbm, exports_hbm, out,
    source, initial, inverse, lift, lift_time, links, orient, exports, load_sem,
    weight_hi, weight_lo, bias, rhs_hi, rhs_lo, state, local, send, top_send, recv, top_recv, send_sem, recv_sem,
    hot, twin_hot, notes, twin_notes, twin_bias, twin_state, feed, twin_top, bulk_send, bulk_recv, ready,
):
    size, elems = source.shape[1:]
    faces = links.shape[0]
    wide = faces * FACE
    peer = exports.shape[1]
    tiles, peer_tiles = elems // LANES, peer // LANES
    hops = ITERS - 1

    space, slab = lax.axis_index("space"), lax.axis_index("slab")
    upper, lower = lax.rem(space + 1, n_space), lax.rem(space + n_space - 1, n_space)
    odd = lax.rem(space, 2)
    has_prev, has_next = slab > 0, slab < n_slab - 1
    even, edge = lax.rem(slab, 2) == 0, space == n_space - 1
    host, home = even & (space == 0), even & edge
    feeder, teller = even & (space == n_space - 2), ~even & edge & has_next
    near_first = even & (space < 2)

    barrier = pltpu.get_barrier_semaphore()
    before, after = lax.rem(slab + n_slab - 1, n_slab), lax.rem(slab + 1, n_slab)
    peers = ((lower, slab), (upper, slab), (space, before), (space, after))
    for k, device in enumerate(peers):
        def greet(device=device):
            pl.semaphore_signal(barrier, inc=1, device_id=device, device_id_type=MESH)

        pl.when(~edge)(greet) if k == 1 else greet()

    @pl.when(host)
    def _():
        pl.semaphore_signal(barrier, inc=1, device_id=(n_space - 2, slab), device_id_type=MESH)

    @pl.when(host & has_prev)
    def _():
        pl.semaphore_signal(barrier, inc=1, device_id=(n_space - 1, before), device_id_type=MESH)

    pairs = (
        (inverse_hbm, inverse), (source_hbm, source), (lift_time_hbm, lift_time), (initial_hbm, initial),
        (exports_hbm, exports), (links_hbm, links), (lift_hbm, lift), (orient_hbm, orient),
    )
    loads = [pltpu.make_async_copy(src, dst, load_sem.at[k]) for k, (src, dst) in enumerate(pairs)]
    for load in loads:
        load.start()

    row = lax.broadcasted_iota(jnp.int32, (size, size), 0)
    at = 64 * ((row >> 1) & 3) + point_of(row >> 3, row & 1)
    pick = (at == lax.broadcasted_iota(jnp.int32, (size, size), 1)).astype(BF16)
    for load in loads[:4]:
        load.wait()
    inv_hi, inv_lo = split(inverse[...])
    own_hi, own_lo = dot(pick, inv_hi).astype(BF16), dot(pick, inv_lo).astype(BF16)
    first_top = jnp.where(slab == 0, initial[...], 0.0)
    top_hi, top_lo = split(first_top)
    lt_hi, lt_lo = split(jnp.concatenate([lift_time[...]] * 2, axis=0))
    time_part = dot_t(own_hi, lt_hi) + dot_t(own_lo, lt_hi) + dot_t(own_hi, lt_lo)
    time_hi = time_part.astype(BF16).astype(F32)
    left = lax.broadcasted_iota(jnp.int32, time_part.shape, 1) < FACE
    time_wide = jnp.concatenate([jnp.where(left, time_hi, time_part - time_hi), time_hi], axis=1).astype(BF16)
    top_wide = jnp.concatenate([top_hi, top_hi, top_lo, jnp.zeros_like(top_hi)], axis=0)
    first = dot3(own_hi, own_lo, source[0]) + dot(time_wide, top_wide)
    bias[:size] = first
    state[...] = first

    def copy(src, dst, sems, at, device):
        return pltpu.make_async_remote_copy(
            src_ref=src, dst_ref=dst, send_sem=sems[0].at[at], recv_sem=sems[1].at[at],
            device_id=device, device_id_type=MESH,
        )

    sems, bulk_sems = (send_sem, recv_sem), (bulk_send, bulk_recv)

    def far(n):
        return copy(send.at[n, odd], recv.at[n, 1 - odd], sems, (n, 0), (jnp.where(odd == 1, upper, lower), slab))

    def near(n):
        return copy(send.at[n, 1 - odd], recv.at[n, odd], sems, (n, 1), (jnp.where(odd == 1, lower, upper), slab))

    def late(n):
        return copy(top_send.at[n], top_recv.at[n], sems, (n, 2), (space, after))

    def feed_twin(n):
        return copy(send.at[n, 1 - odd], feed.at[n], sems, (n, 3), (0, slab))

    def tell_twin(n):
        return copy(top_send.at[n], twin_top.at[n], sems, (n, 4), (0, after))

    def bulk():
        return [copy(x, y, bulk_sems, k, (0, slab)) for k, (x, y) in enumerate(((notes, twin_notes), (bias.at[:size], twin_bias)))]

    def spread(column):
        column = jnp.broadcast_to(column, (8, LANES))
        return column & (LANES - 1), column >> 7

    def taken(x, lane):
        return jnp.take_along_axis(x, lane, axis=1, mode="promise_in_bounds")

    def from_state(state, column):
        lane, tile = spread(column)
        face, part = lax.div(tile, tiles), lax.rem(tile, tiles)
        parts = [part == h for h in range(1, tiles)]
        groups = []
        for v in range(size // 8):
            got = taken(state[8 * v:8 * v + 8, :LANES], lane)
            for h in range(1, tiles):
                got = jnp.where(parts[h - 1], taken(state[8 * v:8 * v + 8, h * LANES:(h + 1) * LANES], lane), got)
            groups.append(got)
        return faced(groups, face)

    def faced(groups, face):
        at_face = [face == f for f in range(1, faces)]
        row_odd = (lax.broadcasted_iota(jnp.int32, (8, LANES), 0) & 1) > 0

        def group(i0, j, k):
            return groups[16 * i0 + 4 * j + k]

        result = []
        for q in range(8):
            flip, a0, b0 = q >> 2, (q >> 1) & 1, q & 1
            b = 2 * (flip ^ b0) + b0
            low, high = 2 * (flip ^ a0) + a0, 2 * (1 ^ flip ^ a0) + a0
            sides = [jnp.where(row_odd, group(i0, high, b), group(i0, low, b)) for i0 in range(2)]
            sides += [group(a0, 0, b), group(a0, 3, b), group(a0, b, 0), group(a0, b, 3)]
            x = sides[0]
            for f in range(1, faces):
                x = jnp.where(at_face[f - 1], sides[f], x)
            result.append(x)
        return result

    def from_peer(block, first, column, held):
        lane, tile = spread(column)
        result = held
        for h in range(peer_tiles):
            here = tile == first + h
            result = [
                jnp.where(here, taken(block[8 * q:8 * q + 8, h * LANES:(h + 1) * LANES], lane), result[q])
                for q in range(8)
            ]
        return result

    def turned(groups, code):
        code = jnp.broadcast_to(code, groups[0].shape)
        odd = (lax.broadcasted_iota(jnp.int32, code.shape, 0) & 1) > 0
        swap, back_a, back_b = (code & 4) > 0, (code & 1) > 0, (code & 2) > 0
        swap_odd, swap_even = swap & odd, swap & ~odd
        mid = []
        for q in range(8):
            flip, a0, b0 = q >> 2, (q >> 1) & 1, q & 1
            even_at, odd_at = flip * 4 + b0 * 2 + a0, (1 - flip) * 4 + b0 * 2 + a0
            mid.append(jnp.where(swap_odd, groups[odd_at], jnp.where(swap_even, groups[even_at], groups[q])))
        mid = [jnp.where(back_a, mid[q ^ 2], mid[q]) for q in range(8)]
        return [jnp.where(back_b, mid[q ^ 1], mid[q]) for q in range(8)]

    def put(ref, spot, groups):
        f, h = spot
        for q in range(8):
            ref[f * FACE + 8 * q:f * FACE + 8 * q + 8, h * LANES:(h + 1) * LANES] = groups[q]

    def held(ref, spot):
        f, h = spot
        return [ref[f * FACE + 8 * q:f * FACE + 8 * q + 8, h * LANES:(h + 1) * LANES] for q in range(8)]

    def at_spot(ref, spot, base=0):
        f, h = spot
        return ref[base + f:base + f + 1, h * LANES:(h + 1) * LANES]

    spots = [(f, h) for f in range(faces) for h in range(tiles)]
    outer = faces * tiles

    def pack_top(state, dst):
        sub = lax.broadcasted_iota(jnp.int32, (8, elems), 0) >> 1
        for w in range(8):
            pack = state[32 * w + 24:32 * w + 32]
            for m in range(3):
                pack = jnp.where(sub == m, pltpu.roll(state[32 * w + 8 * m:32 * w + 8 * m + 8], 2 * m + 2, 0), pack)
            dst[8 * w:8 * w + 8] = pack

    def by_wire(edge_kind, n):
        return jnp.logical_or(jnp.logical_not(edge_kind), n < LAG)

    def send_out(n, far_now=True):
        def start_near():
            near(n).start()
            pl.when(feeder & (n < hops - 1))(lambda: feed_twin(n).start())

        ahead = jnp.where(near_first, 1 - odd, odd)
        for half, is_near in ((ahead, near_first), (1 - ahead, ~near_first)):
            for h in range(peer_tiles):
                cols = slice(h * LANES, (h + 1) * LANES)
                put(send.at[n, half], (0, h), from_state(state, exports[pl.ds(half, 1), cols]))
            pl.when(is_near)(start_near)
            pl.when(~is_near & by_wire(home, n) & far_now)(lambda: far(n).start())
        pack_top(state, top_send.at[n])
        pl.when(has_next)(lambda: late(n).start())
        pl.when(teller & (n < hops - 1))(lambda: tell_twin(n).start())

    def one_hot(links, hot):
        element = lax.broadcasted_iota(jnp.int32, (elems, LANES), 0)
        for f, h in spots:
            if f < BY_MATMUL:
                column = lax.rem(at_spot(links, (f, h)), elems)
                cols = slice(f * elems + h * LANES, f * elems + (h + 1) * LANES)
                hot[:, cols] = (element == column).astype(F32).astype(BF16)

    def gather_own(state, local, links, hot):
        hi, lo = split(state[...])
        for f in range(faces):
            if f < BY_MATMUL:
                eye = hot[:, f * elems:(f + 1) * elems]
                got = dot(hi, eye) + dot(lo, eye)
                for h in range(tiles):
                    groups = [got[8 * v:8 * v + 8, h * LANES:(h + 1) * LANES] for v in range(size // 8)]
                    put(local, (f, h), faced(groups, lax.div(spread(at_spot(links, (f, h)))[1], tiles)))
            else:
                for h in range(tiles):
                    put(local, (f, h), from_state(state, at_spot(links, (f, h))))

    def add_near(local, links, block, first):
        for spot in spots:
            put(local, spot, from_peer(block, first, at_spot(links, spot), held(local, spot)))

    def turned_in(spot, groups):
        f, h = spot
        at, cols = slice(f * FACE, (f + 1) * FACE), slice(h * LANES, (h + 1) * LANES)
        rhs_hi[at, cols], rhs_lo[at, cols] = split(jnp.concatenate(groups, axis=0))

    def add_far(local, links, orient, base, block, first):
        for spot in spots:
            got = from_peer(block, first, at_spot(links, spot), held(local, spot))
            turned_in(spot, turned(got, at_spot(orient, spot, base)))

    def add_top(wait, top):
        @pl.when(has_prev)
        def _():
            wait()
            rhs_hi[wide:], rhs_lo[wide:] = split(top[...])

    def take_in(n):
        def wait(is_near):
            pl.when(is_near)(lambda: near(n).wait_recv())
            pl.when(~is_near & by_wire(host, n))(lambda: far(n).wait_recv())

        near_last = near_first & ((space > 0) | (n >= LAG))
        first_side = jnp.where(near_last, odd, 1 - odd)
        wait(~near_last)
        add_near(local, links, recv.at[n, first_side], outer + first_side * peer_tiles)
        add_top(lambda: late(n).wait_recv(), top_recv.at[n])
        wait(near_last)
        add_far(local, links, orient, 0, recv.at[n, 1 - first_side], outer + (1 - first_side) * peer_tiles)

    def twin_step(n):
        @pl.when(n == 0)
        def _():
            told, biases = bulk()
            told.wait_recv()
            one_hot(twin_notes, twin_hot)
            biases.wait_recv()
            twin_state[...] = twin_bias[...]

        feed_twin(n).wait_recv()
        add_top(lambda: tell_twin(n).wait_recv(), twin_top.at[n])
        hi, lo = split(twin_state[...])
        for f in range(faces):
            if f < BY_MATMUL:
                eye = twin_hot[:, f * elems:(f + 1) * elems]
                got = dot(hi, eye) + dot(lo, eye)
            for h in range(tiles):
                spot = (f, h)
                column = at_spot(twin_notes, spot)
                if f < BY_MATMUL:
                    groups = [got[8 * v:8 * v + 8, h * LANES:(h + 1) * LANES] for v in range(size // 8)]
                    groups = faced(groups, lax.div(spread(column)[1], tiles))
                else:
                    groups = from_state(twin_state, column)
                groups = from_peer(feed.at[n], outer, column, groups)
                groups = from_peer(send.at[n, 0], outer + peer_tiles, column, groups)
                turned_in(spot, turned(groups, at_spot(twin_notes, spot, faces)))
        twin_state[...] = solved(slice(0, size), twin_bias[...])

        @pl.when(n + 1 >= LAG)
        def _():
            for h in range(peer_tiles):
                column = twin_notes[2 * faces:2 * faces + 1, h * LANES:(h + 1) * LANES]
                put(recv.at[n + 1, 0], (0, h), from_state(twin_state, column))

    def solved(at, base):
        x_hi, x_lo = rhs_hi[...], rhs_lo[...]
        return dot(jnp.concatenate([weight_hi[at], weight_lo[at], weight_hi[at]], axis=1), jnp.concatenate([x_hi, x_hi, x_lo], axis=0)) + base

    for load in loads[4:5]:
        load.wait()
    pl.semaphore_wait(barrier, len(peers) + (feeder | teller).astype(jnp.int32) - (space == 0).astype(jnp.int32))

    @pl.when(edge)
    def _():
        pl.semaphore_signal(ready, inc=1, device_id=(0, slab), device_id_type=MESH)

    send_out(0, space > 0)
    for load in loads[5:]:
        load.wait()
    one_hot(links, hot)

    @pl.when(home)
    def _():
        notes[:faces] = links[...]
        notes[faces:2 * faces] = orient[...]
        notes[2 * faces:] = jnp.zeros((16 - 2 * faces, elems), jnp.int32)
        notes[2 * faces:2 * faces + 1, :peer] = exports[1:2]
        for part in bulk():
            part.start()

    place = lax.broadcasted_iota(jnp.int32, (wide, wide), 1)
    t, a, b = node_of(place & 63)
    at = (16 * t + 4 * a + b) * faces + (place >> 6)
    order = (at == lax.broadcasted_iota(jnp.int32, (wide, wide), 0)).astype(BF16)
    place = lax.broadcasted_iota(jnp.int32, (FACE, FACE), 1)
    top_order = (point_of(place >> 1, place & 1) == lax.broadcasted_iota(jnp.int32, (FACE, FACE), 0)).astype(BF16)
    lt_hi, lt_lo = split(lift_time[...].T)
    lt_wide = jnp.concatenate([lt_hi, lt_lo, lt_hi], axis=1)
    total_hi, total_lo = split(source[0] + dot(lt_wide, jnp.concatenate([top_hi, top_hi, top_lo], axis=0)))
    lift_hi, lift_lo = split(lift[...])
    lift_hi = jnp.concatenate([dot(lift_hi, order).astype(BF16), dot(lt_hi, top_order).astype(BF16)], axis=1)
    lift_lo = jnp.concatenate([dot(lift_lo, order).astype(BF16), dot(lt_lo, top_order).astype(BF16)], axis=1)
    inv_hi, inv_lo = jnp.concatenate([own_hi, inv_hi], axis=0), jnp.concatenate([own_lo, inv_lo], axis=0)
    part = dot(inv_hi, lift_hi) + dot(inv_lo, lift_hi) + dot(inv_hi, lift_lo)
    weight_hi[...], weight_lo[...] = split(part)
    bias[size:] = dot(inv_hi[size:], total_hi) + dot(inv_lo[size:], total_hi) + dot(inv_hi[size:], total_lo)
    @pl.when(space == 0)
    def _():
        pl.semaphore_wait(ready, 1)
        far(0).start()

    rhs_hi[wide:] = jnp.zeros((FACE, elems), BF16)
    rhs_lo[wide:] = jnp.zeros((FACE, elems), BF16)

    def sent(n):
        pl.when(by_wire(home, n))(lambda: far(n).wait_send())
        near(n).wait_send()
        pl.when(feeder & (n < hops - 1))(lambda: feed_twin(n).wait_send())
        pl.when(has_next)(lambda: late(n).wait_send())
        pl.when(teller & (n < hops - 1))(lambda: tell_twin(n).wait_send())

    def step(n, carry):
        pl.when(n > 0)(lambda: sent(n - 1))
        gather_own(state, local, links, hot)
        pl.when(host & (n > 0))(lambda: twin_step(n - 1))
        take_in(n)
        state[...] = solved(slice(0, size), bias[:size])
        send_out(n + 1)
        return carry

    lax.fori_loop(0, hops - 1, step, 0)
    sent(hops - 2)
    gather_own(state, local, links, hot)
    pl.when(host)(lambda: twin_step(hops - 2))
    take_in(hops - 1)
    out[0] = solved(slice(size, 2 * size), bias[size:])

    sent(hops - 1)

    @pl.when(home)
    def _():
        for part in bulk():
            part.wait_send()


def body(n_space, n_slab, source, initial, inverse, lift, lift_time, links, orient, exports, counts):
    size, elems = source.shape[1:]
    wide = links.shape[0] * FACE
    depth = wide + FACE
    peer = exports.shape[0] // 2
    hops = ITERS - 1
    operands = (source, initial, inverse, lift, lift_time.T, links, orient, exports.reshape(2, peer))
    result = pl.pallas_call(
        functools.partial(kernel, n_space, n_slab),
        out_shape=pltpu.VMEM(source.shape, F32),
        in_specs=[pl.BlockSpec(memory_space=pltpu.HBM)] * 8,
        out_specs=pl.BlockSpec(memory_space=pltpu.VMEM),
        scratch_shapes=[
            *(pltpu.VMEM(x.shape, x.dtype) for x in operands),
            pltpu.SemaphoreType.DMA((8,)),
            pltpu.VMEM((2 * size, depth), BF16),
            pltpu.VMEM((2 * size, depth), BF16),
            pltpu.VMEM((2 * size, elems), F32),
            pltpu.VMEM((depth, elems), BF16),
            pltpu.VMEM((depth, elems), BF16),
            pltpu.VMEM((size, elems), F32),
            pltpu.VMEM((wide, elems), F32),
            pltpu.VMEM((hops, 2, FACE, peer), F32),
            pltpu.VMEM((hops, FACE, elems), F32),
            pltpu.VMEM((hops, 2, FACE, peer), F32),
            pltpu.VMEM((hops, FACE, elems), F32),
            pltpu.SemaphoreType.DMA((hops, 5)),
            pltpu.SemaphoreType.DMA((hops, 5)),
            pltpu.VMEM((elems, BY_MATMUL * elems), BF16),
            pltpu.VMEM((elems, BY_MATMUL * elems), BF16),
            pltpu.VMEM((16, elems), jnp.int32),
            pltpu.VMEM((16, elems), jnp.int32),
            pltpu.VMEM((size, elems), F32),
            pltpu.VMEM((size, elems), F32),
            pltpu.VMEM((hops, FACE, peer), F32),
            pltpu.VMEM((hops, FACE, elems), F32),
            pltpu.SemaphoreType.DMA((2,)),
            pltpu.SemaphoreType.DMA((2,)),
            pltpu.SemaphoreType.REGULAR,
        ],
        compiler_params=pltpu.CompilerParams(collective_id=0, has_side_effects=True, vmem_limit_bytes=60000 * 1024),
    )(*operands)
    return jnp.where(lax.broadcasted_iota(jnp.int32, result.shape, 2) < counts.reshape(1, 1, 1), result, 0.0)


def solution(mesh):
    return jax.shard_map(
        functools.partial(body, mesh.shape["space"], mesh.shape["slab"]),
        mesh=mesh,
        in_specs=(
            P("slab", None, "space"),
            P(None, "space"),
            P(),
            P(),
            P(),
            P(None, "space"),
            P(None, "space"),
            P("space"),
            P("space"),
        ),
        out_specs=P("slab", None, "space"),
        check_vma=False,
    )
```
